256 devices in a mesh: batch: 32 (over z_hi, y, core), gene: 8 (over x, z_lo).
Axes of the slice: x: 4, y: 4, z: 8 (z_hi: 4, z_lo: 2; z = z_hi * 2 + z_lo), core: 2. Of those that a mesh axis runs over, the one named last changes fastest.
Arguments:
- umi_counts: int32 [32768, 8192], P('batch', 'gene'), may hold values from 0 to 65535
- cell_donors: int32 [32768], P('batch'), may hold values from 0 to 127
- cell_types: int32 [32768], P('batch'), may hold values from 0 to 23
- live_cells: int32 [32], P('batch'), may hold values from 1 to 1024, 20480 in all
- dosages: int32 [128, 4096], P(None, 'batch'), may hold values from 0 to 2
Outputs:
- scores: bfloat16 [24, 8192, 4096], P(None, ('gene', 'batch'))
The draws below stay inside these ranges and needn't reach their ends.
All inputs are finite; a program needn't handle non-finite values. No bound on the sum of `live_cells` on one device may be relied on, other than what follows from the above.
Results may differ from the reference program's by a relative error of at most 0.0069.
Values may be sent and summed in bfloat16 or wider, within the bound.
A program may use at most 128 MiB of HBM per device.

```python
import math
import jax
import jax.numpy as jnp
import numpy as np
from jax import lax

GENES = 8192
TYPES = 24
DONORS = 128
CELL_DEV = 1024
CELLS = 32768
VARIANTS = 4096
N_BATCH = 32


def draw_umi_counts(key, part):
    counts_key = jax.random.fold_in(key, 11)
    depth_key = jax.random.fold_in(key, 23)
    raw_counts = jax.random.randint(counts_key, (CELLS, GENES), 0, 65536, dtype=jnp.int32)
    depth_shift = jax.random.randint(depth_key, (CELLS, 1), 0, 4, dtype=jnp.int32)
    divisor = jnp.left_shift(jnp.ones_like(depth_shift), depth_shift)
    return jnp.floor_divide(raw_counts, divisor).astype(jnp.int32)


def set_ends(drawn, stream_key, smallest, largest):
    index_at = [jax.random.randint(jax.random.fold_in(stream_key, axis), (), 0, length) for axis, length in enumerate(drawn.shape)]
    main_axis = drawn.shape.index(max(drawn.shape))
    neighbour = index_at[:main_axis] + [(index_at[main_axis] + 1) % drawn.shape[main_axis]] + index_at[main_axis + 1:]
    return drawn.at[tuple(index_at)].set(smallest).at[tuple(neighbour)].set(largest)


def cumulative_ranks(count, slope):
    weights = [(1 << 20) // math.isqrt(rank ** slope) + 1 for rank in range(1, count + 1)]
    deviation = 1 + sum(weights) // (1 << 30)
    return np.cumsum(np.array([max(1, weight // deviation) for weight in weights]))


def ranked(key, shape, amount, skew):
    table = cumulative_ranks(amount, skew)
    lot = jax.random.randint(jax.random.fold_in(key, 1), shape, 0, int(table[amount - 1]))
    standing = jnp.searchsorted(jnp.asarray(table, jnp.int32), lot, side="right")
    return jax.random.permutation(jax.random.fold_in(key, 2), amount)[standing].astype(jnp.int32)


def profile(number_of, total, most, lean):
    weights = [(1 << 20) // math.isqrt(rank ** lean) + 1 for rank in range(2, number_of + 1)]
    surplus, holding = total - most - (number_of - 1), [1] * (number_of - 1)
    while surplus > 0:
        movable = [i for i in range(number_of - 1) if holding[i] < most]
        mass, budget = sum([weights[i] for i in movable]), surplus
        for i in movable:
            extra = min(most - holding[i], max(1, budget * weights[i] // mass), surplus)
            holding[i] = holding[i] + extra
            surplus = surplus - extra
    return np.array([most] + holding)


def uneven(rng, count, total, limit, lean):
    if count == 2:
        one = jax.random.randint(rng, (), max(1, total - limit), min(limit, total - 1) + 1)
        return jnp.stack([one, total - one])
    tallies = jnp.asarray(profile(count, total, limit, lean), jnp.int32)
    pairs = (count - 1) // 2
    giver, taker = tallies[1:1 + 2 * pairs:2], tallies[2:2 + 2 * pairs:2]
    room = jnp.minimum(giver - 1, limit - taker)
    moved = jax.random.randint(jax.random.fold_in(rng, 1), (pairs,), 0, 1 << 20) % (room + 1)
    tallies = tallies.at[1:1 + 2 * pairs:2].set(giver - moved).at[2:2 + 2 * pairs:2].set(taker + moved)
    return tallies[jax.random.permutation(jax.random.fold_in(rng, 2), count)]


def setup_inputs(seed: int = 0) -> dict:
    key_list = jax.random.split(jax.random.key(seed), 6)
    umi_counts = draw_umi_counts(jax.random.fold_in(key_list[5], 71), 0)
    cell_donors = set_ends(jax.random.randint(key_list[1], (CELLS,), 0, DONORS), jax.random.fold_in(key_list[1], 1), 0, DONORS - 1).astype(jnp.int32)
    cell_types = set_ends(ranked(key_list[2], (CELLS,), TYPES, 2), jax.random.fold_in(key_list[2], 3), 0, TYPES - 1).astype(jnp.int32)
    live_cells = uneven(key_list[3], N_BATCH, CELLS * 5 // 8, CELL_DEV, 2).astype(jnp.int32)
    dosages = set_ends(jax.random.randint(key_list[4], (DONORS, VARIANTS), 0, 3), jax.random.fold_in(key_list[4], 1), 0, 2).astype(jnp.int32)
    return dict(umi_counts=umi_counts, cell_donors=cell_donors, cell_types=cell_types, live_cells=live_cells, dosages=dosages)


def reference(umi_counts, cell_donors, cell_types, live_cells, dosages):
    cells_total = umi_counts.shape[0]
    total_groups = TYPES * DONORS
    row_index = jnp.arange(cells_total, dtype=jnp.int32)
    alive = row_index % CELL_DEV < live_cells[row_index // CELL_DEV]
    group_ids = jnp.where(alive, cell_types * DONORS + cell_donors, total_groups).astype(jnp.int32)
    rounded = lax.optimization_barrier(umi_counts.astype(jnp.bfloat16)).astype(jnp.float32)
    pseudo = jax.ops.segment_sum(rounded, group_ids, num_segments=total_groups + 1)[:total_groups]
    library = jnp.maximum(lax.optimization_barrier(jnp.sum(pseudo, axis=1)), 1.0)
    logged = jnp.log1p(10000.0 * pseudo / library[:, None]).reshape(TYPES, DONORS, -1)
    centred = logged - lax.optimization_barrier(jnp.mean(logged, axis=1, keepdims=True))
    standard = (centred * lax.rsqrt(lax.optimization_barrier(jnp.mean(centred * centred, axis=1, keepdims=True)) + 1e-06)).astype(jnp.bfloat16)
    genotype = dosages.astype(jnp.float32)
    geno_centred = genotype - lax.optimization_barrier(jnp.mean(genotype, axis=0, keepdims=True))
    geno = (geno_centred * lax.rsqrt(lax.optimization_barrier(jnp.mean(geno_centred * geno_centred, axis=0, keepdims=True)) + 1e-06)).astype(jnp.bfloat16)
    factor = DONORS ** (-0.5)

    def per_type(block):
        return (jnp.dot(block.T, geno, preferred_element_type=jnp.float32) * factor).astype(jnp.bfloat16)
    return lax.map(per_type, standard)
```

```python
import jax
import jax.numpy as jnp
from jax import lax
from jax.experimental import pallas as pl
from jax.experimental.pallas import tpu as pltpu
from jax.sharding import Mesh
from jax.sharding import PartitionSpec as P

TYPES = 24
DONORS = 128
AXES = ("batch_0", "batch_1", "batch_2", "gene_0", "gene_1")
SIZES = {"batch_0": 4, "batch_1": 4, "batch_2": 2, "gene_0": 4, "gene_1": 2}
Z, Y, CORE, X, ZLO = AXES
BATCH = AXES[:3]
GENE = AXES[3:]
MESH = pl.DeviceIdType.MESH
F32 = jnp.float32
BF16 = jnp.bfloat16

CHUNKS = (2, 1, 3, 0)
SLOTS = tuple((dy, dc) for dy in (0, 1, 3, 2) for dc in (0, 1))
ZSLOTS = tuple((oz, ol) for oz in range(4) for ol in range(2))
OFFS = (1, 2, 3)
STRIP = 32
NT = (((1,), (1,)), ((), ()))
TN = (((0,), (0,)), ((), ()))


def three_parts(value):
    first = value.astype(BF16)
    rest = value - first.astype(F32)
    second = rest.astype(BF16)
    third = (rest - second.astype(F32)).astype(BF16)
    return first, second, third


def gather_kernel(
    live_ref, umi_ref, donors_ref, types_ref, dosages_ref,
    std_ref, geno_ref,
    xin, sendb, recvb, codeb, onehot, mask, wide, acc, zsend, zrecv, rows, gown, gbuf, lsend, lrx, lrz, lry,
    in_sem, d_send, d_recv, c_send, c_recv, g_send, g_recv, l_send, l_recv, z_send, z_recv, out_sem,
):
    at = {axis: lax.axis_index(axis) for axis in AXES}
    zi, yi, ci, xi = at[Z], at[Y], at[CORE], at[X]

    def moved(axis, offset):
        return lax.rem(at[axis] + offset, SIZES[axis])

    def peer(**offsets):
        return {axis: moved(axis, offset) for axis, offset in offsets.items() if offset}

    def remote(src, dst, send, recv, device):
        return pltpu.make_async_remote_copy(
            src_ref=src, dst_ref=dst, send_sem=send, recv_sem=recv, device_id=device, device_id_type=MESH
        )

    y_peers = [peer(batch_1=dy, batch_2=dc) for dy, dc in SLOTS]
    z_peers = [peer(batch_0=oz, gene_1=ol) for oz, ol in ZSLOTS]
    x_peers = [peer(gene_0=o) for o in OFFS]

    loads = []
    for c, off in enumerate(CHUNKS):
        col = pl.multiple_of(moved(Z, off) * 256, 256)
        load = pltpu.make_async_copy(umi_ref.at[:, pl.ds(col, 256)], xin.at[c], in_sem.at[c])
        load.start()
        loads.append(load)

    barrier = pltpu.get_barrier_semaphore()
    for device in y_peers[1:] + z_peers[1:] + x_peers:
        pl.semaphore_signal(barrier, inc=1, device_id=device, device_id_type=MESH)

    slot = lax.broadcasted_iota(jnp.int32, (8, 128), 0) * 128 + lax.broadcasted_iota(jnp.int32, (8, 128), 1)
    alive = slot < live_ref[0]
    types = types_ref[...]
    donors = donors_ref[...]
    codeb[0] = jnp.where(alive, ((types >> 3) * DONORS + donors) * 8 + (types & 7), -8)

    genotype = dosages_ref[...].astype(F32)
    centred = genotype - jnp.mean(genotype, axis=0, keepdims=True)
    gown[...] = (centred * lax.rsqrt(jnp.mean(centred * centred, axis=0, keepdims=True) + 1e-06)).astype(BF16)
    quarter = pl.ds(pl.multiple_of(xi * 32, 32), 32)
    gbuf[zi, yi, ci, quarter, :] = gown[quarter, :]
    rows[...] = jnp.zeros_like(rows)
    lane = lax.broadcasted_iota(jnp.int32, (STRIP, 128), 1)
    low = lane < 64
    even = (lane & 32) == 0

    def pack(c):
        def body(i, _):
            r0 = pl.multiple_of(i * STRIP, STRIP)
            total = None
            for h in range(2):
                x = [
                    xin[c, pl.ds(pl.multiple_of(k * 256 + r0, STRIP), STRIP), pl.ds(h * 128, 128)].astype(F32)
                    for k in range(4)
                ]
                a = [None] * 4
                for k in range(2):
                    a[k] = jnp.where(low, x[k], pltpu.roll(x[k + 2], 64, 1))
                    a[k + 2] = jnp.where(low, pltpu.roll(x[k], 64, 1), x[k + 2])
                for k in (0, 2):
                    for q, piece in (
                        (k, jnp.where(even, a[k], pltpu.roll(a[k + 1], 32, 1))),
                        (k + 1, jnp.where(even, pltpu.roll(a[k], 96, 1), a[k + 1])),
                    ):
                        rounded = piece.astype(BF16)
                        sendb[c, h * 4 + q, pl.ds(r0, STRIP), :] = rounded
                        exact = rounded.astype(F32)
                        total = exact if total is None else total + exact
            rows[pl.ds(r0, STRIP), :] += total
            return 0

        lax.fori_loop(0, 256 // STRIP, body, 0)

    own = yi * 2 + ci
    pending = []

    def start(copy):
        copy.start()
        pending.append(copy)
        return copy

    def send_pieces(c):
        for k in (2, 3, 4, 5, 6, 7, 1):
            dy, dc = SLOTS[k]
            piece = moved(Y, dy) * 2 + moved(CORE, dc)
            start(remote(sendb.at[c, piece], recvb.at[c, k], d_send.at[c, k], d_recv.at[c, k], y_peers[k]))

    loads[0].wait()
    pack(0)
    pl.semaphore_wait(barrier, 7 + 7 + 3)
    send_pieces(0)
    code_copies = [
        start(remote(codeb.at[0], codeb.at[k], c_send.at[k], c_recv.at[k], y_peers[k])) for k in range(1, 8)
    ]
    g1 = [
        start(remote(gbuf.at[zi, yi, ci, quarter], gbuf.at[zi, yi, ci, quarter], g_send.at[0, o], g_recv.at[0, o], {Z: moved(Z, off)}))
        for o, off in enumerate(OFFS)
    ]
    loads[1].wait()
    pack(1)
    send_pieces(1)
    for c in (2, 3):
        loads[c].wait()
        pack(c)
    for c in range(4):
        recvb[c, 0] = sendb[c, own]

    select = jnp.where(
        lax.broadcasted_iota(jnp.int32, (8, 128), 1) // 32 == lax.broadcasted_iota(jnp.int32, (8, 128), 0), 1.0, 0.0
    ).astype(BF16)
    sums = sum(lax.dot_general(select, part, NT, preferred_element_type=F32) for part in three_parts(rows[...]))
    part_library = None
    for k in range(4):
        type_row = jnp.concatenate([jnp.where(alive, types, -1)[2 * k + i : 2 * k + i + 1, :] for i in range(2)], axis=1)
        donor_row = jnp.concatenate([donors[2 * k + i : 2 * k + i + 1, :] for i in range(2)], axis=1)
        own_type = lax.broadcasted_iota(jnp.int32, (32, 256), 0) == type_row
        own_donor = jnp.where(lax.broadcasted_iota(jnp.int32, (DONORS, 256), 0) == donor_row, 1.0, 0.0).astype(BF16)
        for part in three_parts(sums[k : k + 1, :]):
            left = jnp.where(own_type, part.astype(F32), 0.0).astype(BF16)
            term = lax.dot_general(left, own_donor, NT, preferred_element_type=F32)
            part_library = term if part_library is None else part_library + term
    lsend[0] = part_library
    lx = [start(remote(lsend.at[0], lrx.at[o], l_send.at[0, o], l_recv.at[0, o], x_peers[o])) for o in range(3)]

    block = lax.broadcasted_iota(jnp.int32, (128, 128), 1) // 32

    def build(s):
        code = codeb[s]
        columns = jnp.transpose((code & 7).astype(F32)).astype(jnp.int32)
        group = code >> 3
        for g in range(8):
            match = lax.broadcasted_iota(jnp.int32, (384, 128), 0) == group[g : g + 1, :]
            onehot[s, :, pl.ds(g * 128, 128)] = jnp.where(match, 1.0, 0.0).astype(BF16)
            column = columns[:, g : g + 1]
            for h in range(2):
                mask[s, pl.ds(g * 128, 128), pl.ds(h * 128, 128)] = jnp.where(column == block + 4 * h, 1.0, 0.0).astype(BF16)

    build(0)
    for copy in g1:
        copy.wait_recv()
    g2 = [
        start(remote(gbuf.at[:, yi, ci, quarter], gbuf.at[:, yi, ci, quarter], g_send.at[1, o], g_recv.at[1, o], {Y: moved(Y, off)}))
        for o, off in enumerate(OFFS)
    ]
    for copy in code_copies:
        copy.wait_recv()
    lax.fori_loop(1, 8, lambda s, _: (build(s), 0)[1], 0)
    send_pieces(2)
    for copy in lx:
        copy.wait_recv()
    lsend[1] = lsend[0] + lrx[0] + lrx[1] + lrx[2]
    lz = [start(remote(lsend.at[1], lrz.at[k], l_send.at[1, k], l_recv.at[1, k], z_peers[k])) for k in range(1, 8)]

    quad = lax.broadcasted_iota(jnp.int32, (STRIP, 128), 1) // 32

    def group_sums(c):
        acc[...] = jnp.zeros_like(acc)

        def body(s, _):
            @pl.when(s > 0)
            def _():
                remote(recvb.at[c, s], recvb.at[c, s], d_send.at[c, s], d_recv.at[c, s], y_peers[1]).wait_recv()

            def widen(i, _):
                r0 = pl.multiple_of(i * STRIP, STRIP)
                x = recvb[c, s, pl.ds(r0, STRIP), :].astype(F32)
                turned = [x] + [pltpu.roll(x, 32 * d, 1) for d in (1, 2, 3)]
                for k in range(4):
                    spread = turned[(3 - k) % 4]
                    for b in range(3):
                        spread = jnp.where(quad == b, turned[(b - k) % 4], spread)
                    spread = spread.astype(BF16)
                    at_rows = pl.ds(pl.multiple_of(k * 256 + r0, STRIP), STRIP)
                    for h in range(2):
                        cols = pl.ds(h * 128, 128)
                        wide[at_rows, cols] = spread * mask[s, at_rows, cols]
                return 0

            lax.fori_loop(0, 256 // STRIP, widen, 0)
            acc[...] += jnp.dot(onehot[s], wide[...], preferred_element_type=F32)
            return 0

        lax.fori_loop(0, 8, body, 0)

    def send_sums(c):
        zsend[c] = acc[...].astype(BF16)
        return start(remote(zsend.at[c], zrecv.at[c], z_send.at[c], z_recv.at[c], {Z: moved(Z, CHUNKS[c])}))

    group_sums(0)
    z_copies = [send_sums(0)]

    for copy in lz:
        copy.wait_recv()
    lsend[2] = lsend[1] + sum(lrz[k] for k in range(1, 8))
    ly = [start(remote(lsend.at[2], lry.at[k], l_send.at[2, k], l_recv.at[2, k], y_peers[k])) for k in range(1, 8)]
    send_pieces(3)
    for copy in g2:
        copy.wait_recv()
    g3 = [
        start(remote(gbuf.at[:, :, ci, quarter], gbuf.at[:, :, ci, quarter], g_send.at[2, o], g_recv.at[2, o], x_peers[o]))
        for o in range(3)
    ]

    group_sums(1)
    z_copies.append(send_sums(1))
    for copy in g3:
        copy.wait_recv()
    g4 = start(remote(gbuf.at[:, :, ci], gbuf.at[:, :, ci], g_send.at[3, 0], g_recv.at[3, 0], {CORE: 1 - ci}))

    group_sums(2)
    z_copies.append(send_sums(2))
    g4.wait_recv()
    geno_out = pltpu.make_async_copy(gbuf, geno_ref, out_sem)
    geno_out.start()

    for copy in ly:
        copy.wait_recv()
    library_parts = three_parts(jnp.maximum(lsend[2] + sum(lry[k] for k in range(1, 8)), 1.0))

    group_sums(3)
    for copy in z_copies:
        copy.wait_recv()
    type_row = lax.broadcasted_iota(jnp.int32, (32, 256), 0)
    tl = lax.broadcasted_iota(jnp.int32, (32, 256), 1) // 32
    for t in range(3):
        at_rows = pl.ds(t * 128, 128)
        expand = jnp.where(type_row == tl + 8 * t, 1.0, 0.0).astype(BF16)
        library = sum(lax.dot_general(part, expand, TN, preferred_element_type=F32) for part in library_parts)
        pseudo = acc[at_rows, :]
        for c in range(3):
            pseudo = pseudo + zrecv[c, at_rows, :].astype(F32)
        logged = jnp.log1p(10000.0 * pseudo / library)
        spread = logged - jnp.mean(logged, axis=0, keepdims=True)
        standard = spread * lax.rsqrt(jnp.mean(spread * spread, axis=0, keepdims=True) + 1e-06)
        std_ref[pl.ds(t * 256, 256), :] = jnp.transpose(standard).astype(BF16)
    geno_out.wait()
    for copy in pending:
        copy.wait_send()


def scores_kernel(std_ref, geno_ref, out_ref):
    geno = jnp.concatenate([geno_ref[i] for i in range(geno_ref.shape[0])], axis=1)
    product = jnp.dot(std_ref[...], geno, preferred_element_type=F32) * DONORS ** (-0.5)
    out_ref[...] = product.astype(BF16)


def on_device(umi_counts, cell_donors, cell_types, live_cells, dosages):
    vmem = pl.BlockSpec(memory_space=pltpu.VMEM)
    hbm = pl.BlockSpec(memory_space=pl.ANY)
    dma = pltpu.SemaphoreType.DMA
    standard, geno = pl.pallas_call(
        gather_kernel,
        name="gather",
        out_shape=(
            jax.ShapeDtypeStruct((768, 128), BF16),
            jax.ShapeDtypeStruct((4, 4, 2, 128, 128), BF16),
        ),
        in_specs=[pl.BlockSpec(memory_space=pltpu.SMEM), hbm, vmem, vmem, vmem],
        out_specs=(vmem, hbm),
        scratch_shapes=[
            pltpu.VMEM((4, 1024, 256), jnp.int32),
            pltpu.VMEM((4, 8, 256, 128), BF16),
            pltpu.VMEM((4, 8, 256, 128), BF16),
            pltpu.VMEM((8, 8, 128), jnp.int32),
            pltpu.VMEM((8, 384, 1024), BF16),
            pltpu.VMEM((8, 1024, 256), BF16),
            pltpu.VMEM((1024, 256), BF16),
            pltpu.VMEM((384, 256), F32),
            pltpu.VMEM((3, 384, 256), BF16),
            pltpu.VMEM((3, 384, 256), BF16),
            pltpu.VMEM((256, 128), F32),
            pltpu.VMEM((128, 128), BF16),
            pltpu.VMEM((4, 4, 2, 128, 128), BF16),
            pltpu.VMEM((3, 32, 128), F32),
            pltpu.VMEM((3, 32, 128), F32),
            pltpu.VMEM((8, 32, 128), F32),
            pltpu.VMEM((8, 32, 128), F32),
            dma((4,)), dma((4, 8)), dma((4, 8)), dma((8,)), dma((8,)), dma((4, 3)), dma((4, 3)),
            dma((3, 8)), dma((3, 8)), dma((3,)), dma((3,)), dma,
        ],
        compiler_params=pltpu.CompilerParams(
            collective_id=0, has_side_effects=True, vmem_limit_bytes=48 * 1024 * 1024
        ),
    )(live_cells, umi_counts, cell_donors.reshape(8, 128), cell_types.reshape(8, 128), dosages)
    geno = geno.reshape(32, 128, 128)
    scores = pl.pallas_call(
        scores_kernel,
        name="scores",
        grid=(8,),
        out_shape=jax.ShapeDtypeStruct((768, 4096), BF16),
        in_specs=[pl.BlockSpec((768, 128), lambda i: (0, 0)), pl.BlockSpec((4, 128, 128), lambda i: (i, 0, 0))],
        out_specs=pl.BlockSpec((768, 512), lambda i: (0, i)),
    )(standard, geno)
    return scores.reshape(TYPES, 32, 4096)


def solution(mesh):
    torus = Mesh(mesh.devices.reshape(*SIZES.values()), AXES)
    return jax.shard_map(
        on_device,
        mesh=torus,
        in_specs=(P(BATCH, GENE), P(BATCH), P(BATCH), P(BATCH), P(None, BATCH)),
        out_specs=P(None, GENE + BATCH, None),
        check_vma=False,
    )
```

```python
import jax
import jax.numpy as jnp
from jax import lax
from jax.experimental import pallas as pl
from jax.experimental.pallas import tpu as pltpu
from jax.sharding import Mesh
from jax.sharding import PartitionSpec as P

TYPES = 24
DONORS = 128
AXES = ("batch_0", "batch_1", "batch_2", "gene_0", "gene_1")
SIZES = {"batch_0": 4, "batch_1": 4, "batch_2": 2, "gene_0": 4, "gene_1": 2}
Z, Y, CORE, X, ZLO = AXES
BATCH = AXES[:3]
GENE = AXES[3:]
MESH = pl.DeviceIdType.MESH
F32 = jnp.float32
BF16 = jnp.bfloat16

BLOCKS = (2, 1, 3, 0)
CODE = 2112.0
LOG2 = 0.6931471805599453
SLOTS = tuple((dy, dc) for dy in (0, 1, 3, 2) for dc in (0, 1))
ZSLOTS = tuple((oz, ol) for oz in range(4) for ol in range(2))
OFFS = (1, 2, 3)
STRIP = 128
COLUMNS = 1024
VMEM_LIMIT = 67043328
NT = (((1,), (1,)), ((), ()))
TN = (((0,), (0,)), ((), ()))


def three_parts(value):
    first = value.astype(BF16)
    rest = value - first.astype(F32)
    second = rest.astype(BF16)
    third = (rest - second.astype(F32)).astype(BF16)
    return first, second, third


def coded(sums):
    return ((jnp.log(1.0 + sums) * (CODE / LOG2) + 0.5).astype(jnp.int32) - 32768).astype(jnp.int16)


def decoded(codes):
    return jnp.exp((codes.astype(jnp.int32) + 32768).astype(F32) * (LOG2 / CODE)) - 1.0


def gather_kernel(
    live_ref, umi_ref, donors_ref, types_ref, dosages_ref,
    std_ref, geno_ref,
    xin, sendb, recvb, codeb, onehot, mask, acc, zsend, zrecv, rows, gown, gbuf, lsend, lrx, lrz, lry,
    in_sem, d_send, d_recv, c_send, c_recv, g_send, g_recv, l_send, l_recv, z_send, z_recv, out_sem,
):
    at = {axis: lax.axis_index(axis) for axis in AXES}
    zi, yi, ci, xi = at[Z], at[Y], at[CORE], at[X]

    def moved(axis, offset):
        return lax.rem(at[axis] + offset, SIZES[axis])

    def peer(**offsets):
        return {axis: moved(axis, offset) for axis, offset in offsets.items() if offset}

    def remote(src, dst, send, recv, device):
        return pltpu.make_async_remote_copy(
            src_ref=src, dst_ref=dst, send_sem=send, recv_sem=recv, device_id=device, device_id_type=MESH
        )

    y_peers = [peer(batch_1=dy, batch_2=dc) for dy, dc in SLOTS]
    z_peers = [peer(batch_0=oz, gene_1=ol) for oz, ol in ZSLOTS]
    x_peers = [peer(gene_0=o) for o in OFFS]

    loads = []
    for c, off in enumerate(BLOCKS):
        col = pl.multiple_of(moved(Z, off) * 256, 256)
        loads.append(pltpu.make_async_copy(umi_ref.at[:, pl.ds(col, 256)], xin.at[c], in_sem.at[c]))
    loads[0].start()

    barrier = pltpu.get_barrier_semaphore()
    for device in y_peers[1:] + z_peers[1:] + x_peers:
        pl.semaphore_signal(barrier, inc=1, device_id=device, device_id_type=MESH)

    slot = lax.broadcasted_iota(jnp.int32, (8, 128), 0) * 128 + lax.broadcasted_iota(jnp.int32, (8, 128), 1)
    alive = slot < live_ref[0]
    types = types_ref[...]
    donors = donors_ref[...]
    codeb[0] = jnp.where(alive, ((types >> 3) * DONORS + donors) * 8 + (types & 7), -8)

    genotype = dosages_ref[...].astype(F32)
    centred = genotype - jnp.mean(genotype, axis=0, keepdims=True)
    gown[...] = (centred * lax.rsqrt(jnp.mean(centred * centred, axis=0, keepdims=True) + 1e-06)).astype(BF16)
    quarter = pl.ds(pl.multiple_of(xi * 32, 32), 32)
    gbuf[zi, yi, ci, quarter, :] = gown[quarter, :]
    rows[...] = jnp.zeros_like(rows)
    lane = lax.broadcasted_iota(jnp.int32, (STRIP, 128), 1)
    low = lane < 64
    even = (lane & 32) == 0
    first = (lane & 16) == 0

    def pack(c):
        def body(i, _):
            r0 = pl.multiple_of(i * STRIP, STRIP)
            total = None
            for h in range(2):
                x = []
                for k in range(4):
                    cells = pl.ds(pl.multiple_of(k * 256 + r0, STRIP), STRIP)
                    value = xin[c, cells, pl.ds(h * 128, 128)]
                    if c in (1, 2):
                        value = jnp.where(first, value, xin[3 - c, cells, pl.ds(h * 128, 128)])
                    x.append(value.astype(F32))
                a = [None] * 4
                for k in range(2):
                    a[k] = jnp.where(low, x[k], pltpu.roll(x[k + 2], 64, 1))
                    a[k + 2] = jnp.where(low, pltpu.roll(x[k], 64, 1), x[k + 2])
                for k in (0, 2):
                    for q, piece in (
                        (k, jnp.where(even, a[k], pltpu.roll(a[k + 1], 32, 1))),
                        (k + 1, jnp.where(even, pltpu.roll(a[k], 96, 1), a[k + 1])),
                    ):
                        rounded = piece.astype(BF16)
                        sendb[c, h * 4 + q, pl.ds(r0, STRIP), :] = rounded
                        exact = rounded.astype(F32)
                        total = exact if total is None else total + exact
            rows[pl.ds(r0, STRIP), :] += total
            return 0

        lax.fori_loop(0, 256 // STRIP, body, 0)

    own = yi * 2 + ci
    pending = []

    def start(copy):
        copy.start()
        pending.append(copy)
        return copy

    def send_pieces(c):
        for k in (2, 3, 4, 5, 6, 7, 1):
            dy, dc = SLOTS[k]
            piece = moved(Y, dy) * 2 + moved(CORE, dc)
            start(remote(sendb.at[c, piece], recvb.at[c, k], d_send.at[c, k], d_recv.at[c, k], y_peers[k]))

    loads[0].wait()
    for c in (1, 2, 3):
        loads[c].start()
    pack(0)
    pl.semaphore_wait(barrier, 7 + 7 + 3)
    code_copies = [
        start(remote(codeb.at[0], codeb.at[k], c_send.at[k], c_recv.at[k], y_peers[k])) for k in range(1, 8)
    ]
    send_pieces(0)
    g1 = [
        start(remote(gbuf.at[zi, yi, ci, quarter], gbuf.at[zi, yi, ci, quarter], g_send.at[0, o], g_recv.at[0, o], {Z: moved(Z, off)}))
        for o, off in enumerate(OFFS)
    ]
    loads[1].wait()
    loads[2].wait()
    pack(1)
    send_pieces(1)
    pack(2)
    loads[3].wait()
    pack(3)
    for c in range(4):
        recvb[c, 0] = sendb[c, own]

    select = jnp.where(
        lax.broadcasted_iota(jnp.int32, (8, 128), 1) // 32 == lax.broadcasted_iota(jnp.int32, (8, 128), 0), 1.0, 0.0
    ).astype(BF16)
    sums = sum(lax.dot_general(select, part, NT, preferred_element_type=F32) for part in three_parts(rows[...]))
    part_library = None
    for k in range(4):
        type_row = jnp.concatenate([jnp.where(alive, types, -1)[2 * k + i : 2 * k + i + 1, :] for i in range(2)], axis=1)
        donor_row = jnp.concatenate([donors[2 * k + i : 2 * k + i + 1, :] for i in range(2)], axis=1)
        own_type = lax.broadcasted_iota(jnp.int32, (32, 256), 0) == type_row
        own_donor = jnp.where(lax.broadcasted_iota(jnp.int32, (DONORS, 256), 0) == donor_row, 1.0, 0.0).astype(BF16)
        for part in three_parts(sums[k : k + 1, :]):
            left = jnp.where(own_type, part.astype(F32), 0.0).astype(BF16)
            term = lax.dot_general(left, own_donor, NT, preferred_element_type=F32)
            part_library = term if part_library is None else part_library + term
    lsend[0] = part_library
    lx = [start(remote(lsend.at[0], lrx.at[o], l_send.at[0, o], l_recv.at[0, o], x_peers[o])) for o in range(3)]

    block = (lax.broadcasted_iota(jnp.int32, (128, 128), 1) // 32).astype(F32).astype(BF16)
    donor_at = lax.broadcasted_iota(jnp.int32, (128, 128), 0).astype(F32).astype(BF16)
    one, zero = jnp.ones((128, 128), BF16), jnp.zeros((128, 128), BF16)

    def down(row):
        return jnp.concatenate([jnp.broadcast_to(row, (16, 128)).astype(BF16)] * 8, axis=0)

    def build(s):
        code = codeb[s]
        columns = jnp.transpose((code & 7).astype(F32))
        donor = ((code >> 3) & 127).astype(F32)
        high = [jnp.where((code >> 10) == t, 1.0, 0.0) for t in range(3)]
        for g in range(8):
            cells = pl.ds(g * 128, 128)
            match = donor_at == down(donor[g : g + 1, :])
            for t in range(3):
                onehot[s, pl.ds(t * 128, 128), cells] = jnp.where(match, down(high[t][g : g + 1, :]), zero)
            column = jnp.broadcast_to(columns[:, g : g + 1], (128, 128)).astype(BF16)
            for h in range(2):
                mask[s, cells, pl.ds(h * 128, 128)] = jnp.where(column == block + 4 * h, one, zero)

    build(0)
    for copy in code_copies:
        copy.wait_recv()
    lax.fori_loop(1, 8, lambda s, _: (build(s), 0)[1], 0)
    for copy in g1:
        copy.wait_recv()
    g2 = [
        start(remote(gbuf.at[:, yi, ci, quarter], gbuf.at[:, yi, ci, quarter], g_send.at[1, o], g_recv.at[1, o], {Y: moved(Y, off)}))
        for o, off in enumerate(OFFS)
    ]
    send_pieces(2)
    for copy in lx:
        copy.wait_recv()
    lsend[1] = lsend[0] + lrx[0] + lrx[1] + lrx[2]
    lz = [start(remote(lsend.at[1], lrz.at[k], l_send.at[1, k], l_recv.at[1, k], z_peers[k])) for k in range(1, 8)]

    quad = (lax.broadcasted_iota(jnp.int32, (256, 128), 1) // 32).astype(F32).astype(BF16)

    def group_sums(c):
        acc[...] = jnp.zeros_like(acc)

        def body(s, _):
            @pl.when(s > 0)
            def _():
                remote(recvb.at[c, s], recvb.at[c, s], d_send.at[c, s], d_recv.at[c, s], y_peers[1]).wait_recv()

            piece = recvb[c, s]
            x = piece.astype(F32)
            turned = [piece] + [pltpu.roll(x, 32 * d, 1).astype(BF16) for d in (1, 2, 3)]
            wide = []
            for k in range(4):
                spread = turned[(3 - k) % 4]
                for b in range(3):
                    spread = jnp.where(quad == b, turned[(b - k) % 4], spread)
                at_rows = pl.ds(k * 256, 256)
                wide.append(jnp.concatenate([spread * mask[s, at_rows, pl.ds(h * 128, 128)] for h in range(2)], axis=1))
            acc[...] += jnp.dot(onehot[s], jnp.concatenate(wide, axis=0), preferred_element_type=F32)
            return 0

        lax.fori_loop(0, 8, body, 0)

    near = (lax.broadcasted_iota(jnp.int32, (384, 128), 1) & 16) == 0

    def send_sums(c):
        lower, upper = acc[:, pl.ds(0, 128)], acc[:, pl.ds(128, 128)]
        a = jnp.where(near, lower, pltpu.roll(upper, 16, 1))
        b = jnp.where(near, pltpu.roll(lower, 112, 1), upper)
        up, down_ = (a, b) if c == 1 else (b, a)
        if c == 2:
            for copy in z_copies[:2]:
                copy.wait_recv()
            up, down_ = up + decoded(zrecv[0, 0]), down_ + decoded(zrecv[0, 1])
        zsend[c, 0] = coded(up)
        zsend[c, 1] = coded(down_)
        for d, off in enumerate((1, 3)):
            z_copies.append(
                start(remote(zsend.at[c, d], zrecv.at[c, d], z_send.at[c, d], z_recv.at[c, d], {Z: moved(Z, off)}))
            )

    z_copies = []
    group_sums(0)
    send_sums(0)

    group_sums(1)
    send_sums(1)
    for copy in lz:
        copy.wait_recv()
    lsend[2] = lsend[1] + sum(lrz[k] for k in range(1, 8))
    ly = [start(remote(lsend.at[2], lry.at[k], l_send.at[2, k], l_recv.at[2, k], y_peers[k])) for k in range(1, 8)]
    send_pieces(3)
    for copy in g2:
        copy.wait_recv()
    g3 = [
        start(remote(gbuf.at[:, :, ci, quarter], gbuf.at[:, :, ci, quarter], g_send.at[2, o], g_recv.at[2, o], x_peers[o]))
        for o in range(3)
    ]

    group_sums(2)
    send_sums(2)

    group_sums(3)
    for copy in g3:
        copy.wait_recv()
    g4 = start(remote(gbuf.at[:, :, ci], gbuf.at[:, :, ci], g_send.at[3, 0], g_recv.at[3, 0], {CORE: 1 - ci}))
    for copy in ly:
        copy.wait_recv()
    library_parts = three_parts(jnp.maximum(lsend[2] + sum(lry[k] for k in range(1, 8)), 1.0))
    g4.wait_recv()
    geno_out = pltpu.make_async_copy(gbuf, geno_ref, out_sem)
    geno_out.start()
    for copy in z_copies[2:]:
        copy.wait_recv()
    type_row = lax.broadcasted_iota(jnp.int32, (32, 256), 0)
    tl = lax.broadcasted_iota(jnp.int32, (32, 256), 1) // 32
    here = near[:128]
    for t in range(3):
        at_rows = pl.ds(t * 128, 128)
        expand = jnp.where(type_row == tl + 8 * t, 1.0, 0.0).astype(BF16)
        library = sum(lax.dot_general(part, expand, TN, preferred_element_type=F32) for part in library_parts)
        a = decoded(zrecv[1, 0, at_rows, :]) + decoded(zrecv[2, 1, at_rows, :])
        b = decoded(zrecv[2, 0, at_rows, :]) + decoded(zrecv[1, 1, at_rows, :])
        others = [jnp.where(here, a, pltpu.roll(b, 16, 1)), jnp.where(here, pltpu.roll(a, 112, 1), b)]
        pseudo = acc[at_rows, :] + jnp.concatenate(others, axis=1)
        logged = jnp.log1p(10000.0 * pseudo / library)
        spread = logged - jnp.mean(logged, axis=0, keepdims=True)
        standard = spread * lax.rsqrt(jnp.mean(spread * spread, axis=0, keepdims=True) + 1e-06)
        std_ref[pl.ds(t * 256, 256), :] = jnp.transpose(standard).astype(BF16)
    geno_out.wait()
    for copy in pending:
        copy.wait_send()


def scores_kernel(std_ref, geno_ref, out_ref, buffer, sem):
    def store(i):
        columns = pl.ds(pl.multiple_of(i * COLUMNS, COLUMNS), COLUMNS)
        return pltpu.make_async_copy(buffer.at[i], out_ref.at[:, columns], sem.at[i])

    def body(i, _):
        count = COLUMNS // 128
        geno = jnp.concatenate([geno_ref[i * count + j] for j in range(count)], axis=1)
        product = jnp.dot(std_ref[...], geno, preferred_element_type=F32) * DONORS ** (-0.5)
        buffer[i] = product.astype(BF16)
        store(i).start()
        return 0

    steps = buffer.shape[0]
    lax.fori_loop(0, steps, body, 0)
    lax.fori_loop(0, steps, lambda i, _: (store(i).wait(), 0)[1], 0)


def on_device(umi_counts, cell_donors, cell_types, live_cells, dosages):
    vmem = pl.BlockSpec(memory_space=pltpu.VMEM)
    hbm = pl.BlockSpec(memory_space=pl.ANY)
    dma = pltpu.SemaphoreType.DMA
    standard, geno = pl.pallas_call(
        gather_kernel,
        name="gather",
        out_shape=(
            jax.ShapeDtypeStruct((768, 128), BF16),
            jax.ShapeDtypeStruct((4, 4, 2, 128, 128), BF16),
        ),
        in_specs=[pl.BlockSpec(memory_space=pltpu.SMEM), hbm, vmem, vmem, vmem],
        out_specs=(vmem, hbm),
        scratch_shapes=[
            pltpu.VMEM((4, 1024, 256), jnp.int32),
            pltpu.VMEM((4, 8, 256, 128), BF16),
            pltpu.VMEM((4, 8, 256, 128), BF16),
            pltpu.VMEM((8, 8, 128), jnp.int32),
            pltpu.VMEM((8, 384, 1024), BF16),
            pltpu.VMEM((8, 1024, 256), BF16),
            pltpu.VMEM((384, 256), F32),
            pltpu.VMEM((3, 2, 384, 128), jnp.int16),
            pltpu.VMEM((3, 2, 384, 128), jnp.int16),
            pltpu.VMEM((256, 128), F32),
            pltpu.VMEM((128, 128), BF16),
            pltpu.VMEM((4, 4, 2, 128, 128), BF16),
            pltpu.VMEM((3, 32, 128), F32),
            pltpu.VMEM((3, 32, 128), F32),
            pltpu.VMEM((8, 32, 128), F32),
            pltpu.VMEM((8, 32, 128), F32),
            dma((4,)), dma((4, 8)), dma((4, 8)), dma((8,)), dma((8,)), dma((4, 3)), dma((4, 3)),
            dma((3, 8)), dma((3, 8)), dma((3, 2)), dma((3, 2)), dma,
        ],
        compiler_params=pltpu.CompilerParams(
            collective_id=0, has_side_effects=True, vmem_limit_bytes=VMEM_LIMIT
        ),
    )(live_cells, umi_counts, cell_donors.reshape(8, 128), cell_types.reshape(8, 128), dosages)
    geno = geno.reshape(32, 128, 128)
    scores = pl.pallas_call(
        scores_kernel,
        name="scores",
        out_shape=jax.ShapeDtypeStruct((768, 4096), BF16),
        in_specs=[vmem, vmem],
        out_specs=hbm,
        scratch_shapes=[pltpu.VMEM((4096 // COLUMNS, 768, COLUMNS), BF16), dma((4096 // COLUMNS,))],
        compiler_params=pltpu.CompilerParams(vmem_limit_bytes=VMEM_LIMIT),
    )(standard, geno)
    return scores.reshape(TYPES, 32, 4096)


def solution(mesh):
    torus = Mesh(mesh.devices.reshape(*SIZES.values()), AXES)
    return jax.shard_map(
        on_device,
        mesh=torus,
        in_specs=(P(BATCH, GENE), P(BATCH), P(BATCH), P(BATCH), P(None, BATCH)),
        out_specs=P(None, GENE + BATCH, None),
        check_vma=False,
    )
```

```python
import jax
import jax.numpy as jnp
from jax import lax
from jax.experimental import pallas as pl
from jax.experimental.pallas import tpu as pltpu
from jax.sharding import Mesh
from jax.sharding import PartitionSpec as P

TYPES = 24
DONORS = 128
AXES = ("batch_0", "batch_1", "batch_2", "gene_0", "gene_1")
SIZES = {"batch_0": 4, "batch_1": 4, "batch_2": 2, "gene_0": 4, "gene_1": 2}
Z, Y, CORE, X, ZLO = AXES
BATCH = AXES[:3]
GENE = AXES[3:]
MESH = pl.DeviceIdType.MESH
F32 = jnp.float32
BF16 = jnp.bfloat16

BLOCKS = (2, 1, 3, 0)
CODE = 2112.0
LOG2 = 0.6931471805599453
SLOTS = tuple((dy, dc) for dy in (0, 2, 1, 3) for dc in (0, 1))
ZSLOTS = tuple((oz, ol) for oz in range(4) for ol in range(2))
OFFS = (1, 2, 3)
STRIP = 128
BANDS = (512, 512, 1024, 1024, 1024)
VMEM_LIMIT = 67043328
NT = (((1,), (1,)), ((), ()))
TN = (((0,), (0,)), ((), ()))


def three_parts(value):
    first = value.astype(BF16)
    rest = value - first.astype(F32)
    second = rest.astype(BF16)
    third = (rest - second.astype(F32)).astype(BF16)
    return first, second, third


def coded(sums):
    return ((jnp.log(1.0 + sums) * (CODE / LOG2) + 0.5).astype(jnp.int32) - 32768).astype(jnp.int16)


def decoded(codes):
    return jnp.exp((codes.astype(jnp.int32) + 32768).astype(F32) * (LOG2 / CODE)) - 1.0


def gather_kernel(
    live_ref, umi_ref, donors_hbm, types_hbm, dosages_hbm,
    std_ref, geno_ref,
    donors_ref, types_ref, dosages_ref, std,
    xin, sendb, recvb, codeb, onehot, mask, acc, zsend, zrecv, rows, gown, gbuf, lsend, lrx, lrc, lrz, lry, half_lib, library,
    in_sem, d_send, d_recv, c_send, c_recv, g_send, g_recv, l_send, l_recv, z_send, z_recv, small_sem, out_sem,
):
    at = {axis: lax.axis_index(axis) for axis in AXES}
    zi, yi, ci, xi = at[Z], at[Y], at[CORE], at[X]

    def moved(axis, offset):
        return lax.rem(at[axis] + offset, SIZES[axis])

    def peer(**offsets):
        return {axis: moved(axis, offset) for axis, offset in offsets.items() if offset}

    def remote(src, dst, send, recv, device):
        return pltpu.make_async_remote_copy(
            src_ref=src, dst_ref=dst, send_sem=send, recv_sem=recv, device_id=device, device_id_type=MESH
        )

    y_peers = [peer(batch_1=dy, batch_2=dc) for dy, dc in SLOTS]
    z_peers = [peer(batch_0=oz, gene_1=ol) for oz, ol in ZSLOTS]
    x_peers = [peer(gene_0=o) for o in OFFS]

    def cells_of(block):
        return pl.ds(pl.multiple_of(block * 128, 128), 128)

    smalls = [
        pltpu.make_async_copy(src, dst, small_sem.at[i])
        for i, (src, dst) in enumerate(
            ((donors_hbm, donors_ref), (types_hbm, types_ref), (dosages_hbm, dosages_ref))
        )
    ]
    for copy in smalls:
        copy.start()
    loads = []
    col = pl.ds(pl.multiple_of(moved(Z, BLOCKS[0]) * 256, 256), 256)
    for i in range(2):
        for k in range(4):
            block = cells_of(2 * k + i)
            loads.append(pltpu.make_async_copy(umi_ref.at[block, col], xin.at[0, block], in_sem.at[4 * i + k]))
    for c in (1, 2, 3):
        col = pl.ds(pl.multiple_of(moved(Z, BLOCKS[c]) * 256, 256), 256)
        loads.append(pltpu.make_async_copy(umi_ref.at[:, col], xin.at[c], in_sem.at[7 + c]))
    for load in loads[:8]:
        load.start()

    barrier = pltpu.get_barrier_semaphore()
    for device in y_peers[1:] + z_peers[1:] + x_peers:
        pl.semaphore_signal(barrier, inc=1, device_id=device, device_id_type=MESH)

    rows[...] = jnp.zeros_like(rows)
    lane = lax.broadcasted_iota(jnp.int32, (STRIP, 128), 1)
    low = lane < 64
    even = (lane & 32) == 0
    first = (lane & 16) == 0

    def pack(c, begin=0, end=2):
        def body(i, _):
            r0 = pl.multiple_of(i * STRIP, STRIP)
            total = None
            for h in range(2):
                x = []
                for k in range(4):
                    cells = pl.ds(pl.multiple_of(k * 256 + r0, STRIP), STRIP)
                    value = xin[c, cells, pl.ds(h * 128, 128)]
                    if c in (1, 2):
                        value = jnp.where(first, value, xin[3 - c, cells, pl.ds(h * 128, 128)])
                    x.append(value.astype(F32))
                a = [None] * 4
                for k in range(2):
                    a[k] = jnp.where(low, x[k], pltpu.roll(x[k + 2], 64, 1))
                    a[k + 2] = jnp.where(low, pltpu.roll(x[k], 64, 1), x[k + 2])
                for k in (0, 2):
                    for q, piece in (
                        (k, jnp.where(even, a[k], pltpu.roll(a[k + 1], 32, 1))),
                        (k + 1, jnp.where(even, pltpu.roll(a[k], 96, 1), a[k + 1])),
                    ):
                        rounded = piece.astype(BF16)
                        sendb[c, h * 4 + q, pl.ds(r0, STRIP), :] = rounded
                        exact = rounded.astype(F32)
                        total = exact if total is None else total + exact
            rows[pl.ds(r0, STRIP), :] += total
            return 0

        lax.fori_loop(begin, end, body, 0)

    own = yi * 2 + ci
    pending = []

    def start(copy):
        copy.start()
        pending.append(copy)
        return copy

    def send_pieces(c):
        for k in (2, 3, 4, 5, 6, 7, 1):
            dy, dc = SLOTS[k]
            piece = moved(Y, dy) * 2 + moved(CORE, dc)
            start(remote(sendb.at[c, piece], recvb.at[c, k], d_send.at[c, k], d_recv.at[c, k], y_peers[k]))

    def send_half(i):
        at_rows = pl.ds(i * 128, 128)
        for k in (2, 3, 4, 5, 6, 7, 1):
            dy, dc = SLOTS[k]
            piece = moved(Y, dy) * 2 + moved(CORE, dc)
            start(
                remote(sendb.at[0, piece, at_rows], recvb.at[0, k, at_rows], d_send.at[4 * i, k], d_recv.at[4 * i, k], y_peers[k])
            )

    for load in loads[:4]:
        load.wait()
    for load in loads[8:]:
        load.start()
    pack(0, 0, 1)
    for copy in smalls:
        copy.wait()
    slot = lax.broadcasted_iota(jnp.int32, (8, 128), 0) * 128 + lax.broadcasted_iota(jnp.int32, (8, 128), 1)
    alive = slot < live_ref[0]
    types = types_ref[...]
    donors = donors_ref[...]
    codeb[0] = jnp.where(alive, ((types >> 3) * DONORS + donors) * 8 + (types & 7), -8)

    genotype = dosages_ref[...].astype(F32)
    centred = genotype - jnp.mean(genotype, axis=0, keepdims=True)
    gown[...] = (centred * lax.rsqrt(jnp.mean(centred * centred, axis=0, keepdims=True) + 1e-06)).astype(BF16)
    quarter = pl.ds(pl.multiple_of(xi * 32, 32), 32)
    gbuf[zi, yi, ci, quarter, :] = gown[quarter, :]
    pl.semaphore_wait(barrier, 7 + 7 + 3)
    code_copies = [
        start(remote(codeb.at[0], codeb.at[k], c_send.at[k], c_recv.at[k], y_peers[k])) for k in range(1, 8)
    ]
    g1 = [
        start(remote(gbuf.at[zi, yi, ci, quarter], gbuf.at[zi, yi, ci, quarter], g_send.at[0, o], g_recv.at[0, o], {Y: moved(Y, off)}))
        for o, off in enumerate(OFFS)
    ]
    send_half(0)
    for load in loads[4:8]:
        load.wait()
    pack(0, 1, 2)
    send_half(1)
    loads[8].wait()
    loads[9].wait()
    pack(1)
    send_pieces(1)
    pack(2)
    send_pieces(2)
    loads[10].wait()
    pack(3)
    for c in range(4):
        recvb[c, 0] = sendb[c, own]

    select = jnp.where(
        lax.broadcasted_iota(jnp.int32, (8, 128), 1) // 32 == lax.broadcasted_iota(jnp.int32, (8, 128), 0), 1.0, 0.0
    ).astype(BF16)
    sums = sum(lax.dot_general(select, part, NT, preferred_element_type=F32) for part in three_parts(rows[...]))
    part_library = None
    for k in range(4):
        type_row = jnp.concatenate([jnp.where(alive, types, -1)[2 * k + i : 2 * k + i + 1, :] for i in range(2)], axis=1)
        donor_row = jnp.concatenate([donors[2 * k + i : 2 * k + i + 1, :] for i in range(2)], axis=1)
        own_type = lax.broadcasted_iota(jnp.int32, (32, 256), 0) == type_row
        own_donor = jnp.where(lax.broadcasted_iota(jnp.int32, (DONORS, 256), 0) == donor_row, 1.0, 0.0).astype(BF16)
        for part in three_parts(sums[k : k + 1, :]):
            left = jnp.where(own_type, part.astype(F32), 0.0).astype(BF16)
            term = lax.dot_general(left, own_donor, NT, preferred_element_type=F32)
            part_library = term if part_library is None else part_library + term
    lsend[0] = part_library
    lx = [start(remote(lsend.at[0], lrx.at[o], l_send.at[0, o], l_recv.at[0, o], x_peers[o])) for o in range(3)]

    block = (lax.broadcasted_iota(jnp.int32, (128, 128), 1) // 32).astype(F32).astype(BF16)
    donor_at = lax.broadcasted_iota(jnp.int32, (128, 128), 0).astype(F32).astype(BF16)
    one, zero = jnp.ones((128, 128), BF16), jnp.zeros((128, 128), BF16)

    def down(row):
        return jnp.concatenate([jnp.broadcast_to(row, (16, 128)).astype(BF16)] * 8, axis=0)

    def build(s):
        code = codeb[s]
        columns = jnp.transpose((code & 7).astype(F32))
        donor = ((code >> 3) & 127).astype(F32)
        high = [jnp.where((code >> 10) == t, 1.0, 0.0) for t in range(3)]
        for g in range(8):
            cells = pl.ds(g * 128, 128)
            match = donor_at == down(donor[g : g + 1, :])
            for t in range(3):
                onehot[s, pl.ds(t * 128, 128), cells] = jnp.where(match, down(high[t][g : g + 1, :]), zero)
            column = jnp.broadcast_to(columns[:, g : g + 1], (128, 128)).astype(BF16)
            for h in range(2):
                mask[s, cells, pl.ds(h * 128, 128)] = jnp.where(column == block + 4 * h, one, zero)

    build(0)
    for copy in g1:
        copy.wait_recv()
    g2 = [
        start(remote(gbuf.at[zi, :, ci, quarter], gbuf.at[zi, :, ci, quarter], g_send.at[1, o], g_recv.at[1, o], {Z: moved(Z, off)}))
        for o, off in enumerate(OFFS)
    ]
    for copy in code_copies:
        copy.wait_recv()
    lax.fori_loop(1, 8, lambda s, _: (build(s), 0)[1], 0)
    for copy in lx:
        copy.wait_recv()
    lsend[1] = lsend[0] + lrx[0] + lrx[1] + lrx[2]
    lc = start(remote(lsend.at[1], lrc, l_send.at[0, 3], l_recv.at[0, 3], {CORE: 1 - ci}))
    half = pl.ds(pl.multiple_of(ci * 16, 16), 16)

    quad = (lax.broadcasted_iota(jnp.int32, (256, 128), 1) // 32).astype(F32).astype(BF16)

    def group_sums(c, begin=0, end=8):
        if begin == 0:
            acc[...] = jnp.zeros_like(acc)

        def body(s, _):
            @pl.when(s > 0)
            def _():
                if c == 0:
                    for i in range(2):
                        part = recvb.at[0, s, pl.ds(i * 128, 128)]
                        remote(part, part, d_send.at[4 * i, s], d_recv.at[4 * i, s], y_peers[1]).wait_recv()
                else:
                    remote(recvb.at[c, s], recvb.at[c, s], d_send.at[c, s], d_recv.at[c, s], y_peers[1]).wait_recv()

            piece = recvb[c, s]
            x = piece.astype(F32)
            turned = [piece] + [pltpu.roll(x, 32 * d, 1).astype(BF16) for d in (1, 2, 3)]
            wide = []
            for k in range(4):
                spread = turned[(3 - k) % 4]
                for b in range(3):
                    spread = jnp.where(quad == b, turned[(b - k) % 4], spread)
                at_rows = pl.ds(k * 256, 256)
                wide.append(jnp.concatenate([spread * mask[s, at_rows, pl.ds(h * 128, 128)] for h in range(2)], axis=1))
            acc[...] += jnp.dot(onehot[s], jnp.concatenate(wide, axis=0), preferred_element_type=F32)
            return 0

        lax.fori_loop(begin, end, body, 0)

    near = (lax.broadcasted_iota(jnp.int32, (384, 128), 1) & 16) == 0

    def send_sums(c):
        lower, upper = acc[:, pl.ds(0, 128)], acc[:, pl.ds(128, 128)]
        a = jnp.where(near, lower, pltpu.roll(upper, 16, 1))
        b = jnp.where(near, pltpu.roll(lower, 112, 1), upper)
        up, down_ = (a, b) if c == 1 else (b, a)
        if c == 2:
            for copy in z_copies[:2]:
                copy.wait_recv()
            up, down_ = up + decoded(zrecv[0, 0]), down_ + decoded(zrecv[0, 1])
        zsend[c, 0] = coded(up)
        zsend[c, 1] = coded(down_)
        for d, off in enumerate((1, 3)):
            z_copies.append(
                start(remote(zsend.at[c, d], zrecv.at[c, d], z_send.at[c, d], z_recv.at[c, d], {Z: moved(Z, off)}))
            )

    z_copies = []
    group_sums(0, 0, 4)
    lc.wait_recv()
    lsend[2] = lsend[1] + lrc[...]
    lz = [start(remote(lsend.at[2, half], lrz.at[k], l_send.at[1, k], l_recv.at[1, k], z_peers[k])) for k in range(1, 8)]
    group_sums(0, 4, 8)
    send_sums(0)
    for copy in g2:
        copy.wait_recv()
    g3 = [
        start(remote(gbuf.at[:, :, ci, quarter], gbuf.at[:, :, ci, quarter], g_send.at[2, o], g_recv.at[2, o], x_peers[o]))
        for o in range(3)
    ]

    group_sums(1)
    send_sums(1)
    for copy in lz:
        copy.wait_recv()
    half_lib[...] = lsend[2, half, :] + sum(lrz[k] for k in range(1, 8))
    ly = [
        start(remote(half_lib, lry.at[o], l_send.at[2, o], l_recv.at[2, o], {Y: moved(Y, off)}))
        for o, off in enumerate(OFFS)
    ]
    send_pieces(3)

    group_sums(2)
    send_sums(2)
    for copy in g3:
        copy.wait_recv()
    g4 = start(remote(gbuf.at[:, :, ci], gbuf.at[:, :, ci], g_send.at[3, 0], g_recv.at[3, 0], {CORE: 1 - ci}))

    group_sums(3, 0, 4)
    for copy in ly:
        copy.wait_recv()
    library[half, :] = half_lib[...] + lry[0] + lry[1] + lry[2]
    ll = start(remote(library.at[half], library.at[half], l_send.at[2, 3], l_recv.at[2, 3], {CORE: 1 - ci}))
    group_sums(3, 4, 8)
    ll.wait_recv()
    library_parts = three_parts(jnp.maximum(library[...], 1.0))
    g4.wait_recv()
    geno_out = pltpu.make_async_copy(gbuf, geno_ref, out_sem.at[3])
    geno_out.start()
    for copy in z_copies[2:]:
        copy.wait_recv()
    type_row = lax.broadcasted_iota(jnp.int32, (32, 256), 0)
    tl = lax.broadcasted_iota(jnp.int32, (32, 256), 1) // 32
    here = near[:128]
    stores = [geno_out]

    def std_store(t):
        at_rows = pl.ds(t * 256, 256)
        return pltpu.make_async_copy(std.at[at_rows], std_ref.at[at_rows], out_sem.at[t])

    for t in range(3):
        at_rows = pl.ds(t * 128, 128)
        expand = jnp.where(type_row == tl + 8 * t, 1.0, 0.0).astype(BF16)
        size = sum(lax.dot_general(part, expand, TN, preferred_element_type=F32) for part in library_parts)
        a = decoded(zrecv[1, 0, at_rows, :]) + decoded(zrecv[2, 1, at_rows, :])
        b = decoded(zrecv[2, 0, at_rows, :]) + decoded(zrecv[1, 1, at_rows, :])
        others = [jnp.where(here, a, pltpu.roll(b, 16, 1)), jnp.where(here, pltpu.roll(a, 112, 1), b)]
        pseudo = acc[at_rows, :] + jnp.concatenate(others, axis=1)
        logged = jnp.log1p(10000.0 * pseudo / size)
        spread = logged - jnp.mean(logged, axis=0, keepdims=True)
        standard = spread * lax.rsqrt(jnp.mean(spread * spread, axis=0, keepdims=True) + 1e-06)
        std[pl.ds(t * 256, 256), :] = jnp.transpose(standard).astype(BF16)
        stores.append(std_store(t))
        stores[-1].start()
    for copy in stores:
        copy.wait()
    for copy in pending:
        copy.wait_send()


def scores_kernel(std_hbm, geno_hbm, out_ref, std_ref, geno_ref, buffer, in_sem, sem):
    loads = [pltpu.make_async_copy(std_hbm, std_ref, in_sem.at[len(BANDS)])]
    stores = []
    begin = 0
    for i, width in enumerate(BANDS):
        blocks = pl.ds(begin // 128, width // 128)
        loads.append(pltpu.make_async_copy(geno_hbm.at[blocks], geno_ref.at[blocks], in_sem.at[i]))
        columns = pl.ds(begin, width)
        stores.append(pltpu.make_async_copy(buffer.at[:, columns], out_ref.at[:, columns], sem.at[i]))
        begin += width
    for copy in loads:
        copy.start()
    loads[0].wait()
    begin = 0
    for i, width in enumerate(BANDS):
        loads[i + 1].wait()
        geno = jnp.concatenate([geno_ref[begin // 128 + j] for j in range(width // 128)], axis=1)
        product = jnp.dot(std_ref[...], geno, preferred_element_type=F32) * DONORS ** (-0.5)
        buffer[:, pl.ds(begin, width)] = product.astype(BF16)
        stores[i].start()
        begin += width
    for copy in stores:
        copy.wait()


def on_device(umi_counts, cell_donors, cell_types, live_cells, dosages):
    hbm = pl.BlockSpec(memory_space=pl.ANY)
    dma = pltpu.SemaphoreType.DMA
    standard, geno = pl.pallas_call(
        gather_kernel,
        name="gather",
        out_shape=(
            jax.ShapeDtypeStruct((768, 128), BF16),
            jax.ShapeDtypeStruct((4, 4, 2, 128, 128), BF16),
        ),
        in_specs=[pl.BlockSpec(memory_space=pltpu.SMEM)] + [hbm] * 4,
        out_specs=(hbm, hbm),
        scratch_shapes=[
            pltpu.VMEM((8, 128), jnp.int32),
            pltpu.VMEM((8, 128), jnp.int32),
            pltpu.VMEM((DONORS, 128), jnp.int32),
            pltpu.VMEM((768, 128), BF16),
            pltpu.VMEM((4, 1024, 256), jnp.int32),
            pltpu.VMEM((4, 8, 256, 128), BF16),
            pltpu.VMEM((4, 8, 256, 128), BF16),
            pltpu.VMEM((8, 8, 128), jnp.int32),
            pltpu.VMEM((8, 384, 1024), BF16),
            pltpu.VMEM((8, 1024, 256), BF16),
            pltpu.VMEM((384, 256), F32),
            pltpu.VMEM((3, 2, 384, 128), jnp.int16),
            pltpu.VMEM((3, 2, 384, 128), jnp.int16),
            pltpu.VMEM((256, 128), F32),
            pltpu.VMEM((128, 128), BF16),
            pltpu.VMEM((4, 4, 2, 128, 128), BF16),
            pltpu.VMEM((3, 32, 128), F32),
            pltpu.VMEM((3, 32, 128), F32),
            pltpu.VMEM((32, 128), F32),
            pltpu.VMEM((8, 16, 128), F32),
            pltpu.VMEM((3, 16, 128), F32),
            pltpu.VMEM((16, 128), F32),
            pltpu.VMEM((32, 128), F32),
            dma((11,)), dma((5, 8)), dma((5, 8)), dma((8,)), dma((8,)), dma((4, 3)), dma((4, 3)),
            dma((3, 8)), dma((3, 8)), dma((3, 2)), dma((3, 2)), dma((3,)), dma((4,)),
        ],
        compiler_params=pltpu.CompilerParams(
            collective_id=0, has_side_effects=True, vmem_limit_bytes=VMEM_LIMIT
        ),
    )(live_cells, umi_counts, cell_donors.reshape(8, 128), cell_types.reshape(8, 128), dosages)
    geno = geno.reshape(32, 128, 128)
    scores = pl.pallas_call(
        scores_kernel,
        name="scores",
        out_shape=jax.ShapeDtypeStruct((768, 4096), BF16),
        in_specs=[hbm, hbm],
        out_specs=hbm,
        scratch_shapes=[
            pltpu.VMEM((768, 128), BF16),
            pltpu.VMEM((32, 128, 128), BF16),
            pltpu.VMEM((768, 4096), BF16),
            dma((len(BANDS) + 1,)), dma((len(BANDS),)),
        ],
        compiler_params=pltpu.CompilerParams(vmem_limit_bytes=VMEM_LIMIT),
    )(standard, geno)
    return scores.reshape(TYPES, 32, 4096)


def solution(mesh):
    torus = Mesh(mesh.devices.reshape(*SIZES.values()), AXES)
    return jax.shard_map(
        on_device,
        mesh=torus,
        in_specs=(P(BATCH, GENE), P(BATCH), P(BATCH), P(BATCH), P(None, BATCH)),
        out_specs=P(None, GENE + BATCH, None),
        check_vma=False,
    )
```

```python
import jax
import jax.numpy as jnp
from jax import lax
from jax.experimental import pallas as pl
from jax.experimental.pallas import tpu as pltpu
from jax.sharding import Mesh
from jax.sharding import PartitionSpec as P

TYPES = 24
DONORS = 128
AXES = ("batch_0", "batch_1", "batch_2", "gene_0", "gene_1")
SIZES = {"batch_0": 4, "batch_1": 4, "batch_2": 2, "gene_0": 4, "gene_1": 2}
Z, Y, CORE, X, ZLO = AXES
BATCH = AXES[:3]
GENE = AXES[3:]
MESH = pl.DeviceIdType.MESH
F32 = jnp.float32
BF16 = jnp.bfloat16

BLOCKS = (2, 1, 3, 0)
CODE = 2112.0
LOG2 = 0.6931471805599453
SLOTS = tuple((dy, dc) for dy in (0, 2, 1, 3) for dc in (0, 1))
ZSLOTS = tuple((oz, ol) for oz in range(4) for ol in range(2))
OFFS = (1, 2, 3)
STRIP = 128
BANDS = (512, 512, 1024, 1024, 1024)
VMEM_LIMIT = 67043328
NT = (((1,), (1,)), ((), ()))
TN = (((0,), (0,)), ((), ()))


def three_parts(value):
    first = value.astype(BF16)
    rest = value - first.astype(F32)
    second = rest.astype(BF16)
    third = (rest - second.astype(F32)).astype(BF16)
    return first, second, third


def coded(sums):
    return ((jnp.log(1.0 + sums) * (CODE / LOG2) + 0.5).astype(jnp.int32) - 32768).astype(jnp.int16)


def decoded(codes):
    return jnp.exp((codes.astype(jnp.int32) + 32768).astype(F32) * (LOG2 / CODE)) - 1.0


def gather_kernel(
    live_ref, umi_ref, donors_hbm, types_hbm, dosages_hbm,
    std_ref, geno_ref,
    donors_ref, types_ref, dosages_ref, std,
    xin, sendb, recvb, codeb, onehot, mask, acc, zsend, zrecv, rows, gown, gbuf, lsend, lrx, lrc, lrz, lry, half_lib, library, scale,
    in_sem, d_send, d_recv, c_send, c_recv, g_send, g_recv, l_send, l_recv, z_send, z_recv, small_sem, out_sem,
):
    at = {axis: lax.axis_index(axis) for axis in AXES}
    zi, yi, ci, xi = at[Z], at[Y], at[CORE], at[X]

    def moved(axis, offset):
        return lax.rem(at[axis] + offset, SIZES[axis])

    def peer(**offsets):
        return {axis: moved(axis, offset) for axis, offset in offsets.items() if offset}

    def remote(src, dst, send, recv, device):
        return pltpu.make_async_remote_copy(
            src_ref=src, dst_ref=dst, send_sem=send, recv_sem=recv, device_id=device, device_id_type=MESH
        )

    y_peers = [peer(batch_1=dy, batch_2=dc) for dy, dc in SLOTS]
    z_peers = [peer(batch_0=oz, gene_1=ol) for oz, ol in ZSLOTS]
    x_peers = [peer(gene_0=o) for o in OFFS]

    def cells_of(block):
        return pl.ds(pl.multiple_of(block * 128, 128), 128)

    smalls = [
        pltpu.make_async_copy(src, dst, small_sem.at[i])
        for i, (src, dst) in enumerate(
            ((donors_hbm, donors_ref), (types_hbm, types_ref), (dosages_hbm, dosages_ref))
        )
    ]
    for copy in smalls:
        copy.start()
    loads = []
    col = pl.ds(pl.multiple_of(moved(Z, BLOCKS[0]) * 256, 256), 256)
    for i in range(2):
        for k in range(4):
            block = cells_of(2 * k + i)
            loads.append(pltpu.make_async_copy(umi_ref.at[block, col], xin.at[0, block], in_sem.at[4 * i + k]))
    for c in (1, 2, 3):
        col = pl.ds(pl.multiple_of(moved(Z, BLOCKS[c]) * 256, 256), 256)
        loads.append(pltpu.make_async_copy(umi_ref.at[:, col], xin.at[c], in_sem.at[7 + c]))
    for load in loads[:8]:
        load.start()

    barrier = pltpu.get_barrier_semaphore()
    for device in y_peers[1:] + z_peers[1:] + x_peers:
        pl.semaphore_signal(barrier, inc=1, device_id=device, device_id_type=MESH)

    rows[...] = jnp.zeros_like(rows)
    lane = lax.broadcasted_iota(jnp.int32, (STRIP, 128), 1)
    low = lane < 64
    even = (lane & 32) == 0
    first = (lane & 16) == 0

    def pack(c, begin=0, end=2):
        def body(i, _):
            r0 = pl.multiple_of(i * STRIP, STRIP)
            total = None
            for h in range(2):
                x = []
                for k in range(4):
                    cells = pl.ds(pl.multiple_of(k * 256 + r0, STRIP), STRIP)
                    value = xin[c, cells, pl.ds(h * 128, 128)]
                    if c in (1, 2):
                        value = jnp.where(first, value, xin[3 - c, cells, pl.ds(h * 128, 128)])
                    x.append(value.astype(F32))
                a = [None] * 4
                for k in range(2):
                    a[k] = jnp.where(low, x[k], pltpu.roll(x[k + 2], 64, 1))
                    a[k + 2] = jnp.where(low, pltpu.roll(x[k], 64, 1), x[k + 2])
                for k in (0, 2):
                    for q, piece in (
                        (k, jnp.where(even, a[k], pltpu.roll(a[k + 1], 32, 1))),
                        (k + 1, jnp.where(even, pltpu.roll(a[k], 96, 1), a[k + 1])),
                    ):
                        rounded = piece.astype(BF16)
                        sendb[c, h * 4 + q, pl.ds(r0, STRIP), :] = rounded
                        exact = rounded.astype(F32)
                        total = exact if total is None else total + exact
            rows[pl.ds(r0, STRIP), :] += total
            return 0

        lax.fori_loop(begin, end, body, 0)

    own = yi * 2 + ci
    pending = []

    def start(copy):
        copy.start()
        pending.append(copy)
        return copy

    def send_pieces(c):
        for k in (2, 3, 4, 5, 6, 7, 1):
            dy, dc = SLOTS[k]
            piece = moved(Y, dy) * 2 + moved(CORE, dc)
            start(remote(sendb.at[c, piece], recvb.at[c, k], d_send.at[c, k], d_recv.at[c, k], y_peers[k]))

    def send_half(i):
        at_rows = pl.ds(i * 128, 128)
        for k in (2, 3, 4, 5, 6, 7, 1):
            dy, dc = SLOTS[k]
            piece = moved(Y, dy) * 2 + moved(CORE, dc)
            start(
                remote(sendb.at[0, piece, at_rows], recvb.at[0, k, at_rows], d_send.at[4 * i, k], d_recv.at[4 * i, k], y_peers[k])
            )

    for load in loads[:4]:
        load.wait()
    for load in loads[8:]:
        load.start()
    pack(0, 0, 1)
    for copy in smalls:
        copy.wait()
    slot = lax.broadcasted_iota(jnp.int32, (8, 128), 0) * 128 + lax.broadcasted_iota(jnp.int32, (8, 128), 1)
    alive = slot < live_ref[0]
    types = types_ref[...]
    donors = donors_ref[...]
    codeb[0] = jnp.where(alive, ((types >> 3) * DONORS + donors) * 8 + (types & 7), -8)

    genotype = dosages_ref[...].astype(F32)
    centred = genotype - jnp.mean(genotype, axis=0, keepdims=True)
    gown[...] = (centred * lax.rsqrt(jnp.mean(centred * centred, axis=0, keepdims=True) + 1e-06)).astype(BF16)
    quarter = pl.ds(pl.multiple_of(xi * 32, 32), 32)
    gbuf[zi, yi, ci, quarter, :] = gown[quarter, :]
    pl.semaphore_wait(barrier, 7 + 7 + 3)
    code_copies = [
        start(remote(codeb.at[0], codeb.at[k], c_send.at[k], c_recv.at[k], y_peers[k])) for k in range(1, 8)
    ]
    g1 = [
        start(remote(gbuf.at[zi, yi, ci, quarter], gbuf.at[zi, yi, ci, quarter], g_send.at[0, o], g_recv.at[0, o], {Y: moved(Y, off)}))
        for o, off in enumerate(OFFS)
    ]
    send_half(0)
    for load in loads[4:8]:
        load.wait()
    pack(0, 1, 2)
    send_half(1)
    loads[8].wait()
    loads[9].wait()
    pack(1)
    send_pieces(1)
    pack(2)
    send_pieces(2)
    loads[10].wait()
    pack(3)
    for c in range(4):
        recvb[c, 0] = sendb[c, own]

    select = jnp.where(
        lax.broadcasted_iota(jnp.int32, (8, 128), 1) // 32 == lax.broadcasted_iota(jnp.int32, (8, 128), 0), 1.0, 0.0
    ).astype(BF16)
    sums = sum(lax.dot_general(select, part, NT, preferred_element_type=F32) for part in three_parts(rows[...]))
    part_library = None
    for k in range(4):
        type_row = jnp.concatenate([jnp.where(alive, types, -1)[2 * k + i : 2 * k + i + 1, :] for i in range(2)], axis=1)
        donor_row = jnp.concatenate([donors[2 * k + i : 2 * k + i + 1, :] for i in range(2)], axis=1)
        own_type = lax.broadcasted_iota(jnp.int32, (32, 256), 0) == type_row
        own_donor = jnp.where(lax.broadcasted_iota(jnp.int32, (DONORS, 256), 0) == donor_row, 1.0, 0.0).astype(BF16)
        for part in three_parts(sums[k : k + 1, :]):
            left = jnp.where(own_type, part.astype(F32), 0.0).astype(BF16)
            term = lax.dot_general(left, own_donor, NT, preferred_element_type=F32)
            part_library = term if part_library is None else part_library + term
    lsend[0] = part_library
    lx = [start(remote(lsend.at[0], lrx.at[o], l_send.at[0, o], l_recv.at[0, o], x_peers[o])) for o in range(3)]

    block = (lax.broadcasted_iota(jnp.int32, (128, 128), 1) // 32).astype(F32).astype(BF16)
    donor_at = lax.broadcasted_iota(jnp.int32, (128, 128), 0).astype(F32).astype(BF16)
    one, zero = jnp.ones((128, 128), BF16), jnp.zeros((128, 128), BF16)

    def down(row):
        return jnp.concatenate([jnp.broadcast_to(row, (16, 128)).astype(BF16)] * 8, axis=0)

    def build(s):
        code = codeb[s]
        columns = jnp.transpose((code & 7).astype(F32))
        donor = ((code >> 3) & 127).astype(F32)
        high = [jnp.where((code >> 10) == t, 1.0, 0.0) for t in range(3)]
        for g in range(8):
            cells = pl.ds(g * 128, 128)
            match = donor_at == down(donor[g : g + 1, :])
            for t in range(3):
                onehot[s, pl.ds(t * 128, 128), cells] = jnp.where(match, down(high[t][g : g + 1, :]), zero)
            column = jnp.broadcast_to(columns[:, g : g + 1], (128, 128)).astype(BF16)
            for h in range(2):
                mask[s, cells, pl.ds(h * 128, 128)] = jnp.where(column == block + 4 * h, one, zero)

    build(0)
    for copy in g1:
        copy.wait_recv()
    g2 = [
        start(remote(gbuf.at[zi, :, ci, quarter], gbuf.at[zi, :, ci, quarter], g_send.at[1, o], g_recv.at[1, o], {Z: moved(Z, off)}))
        for o, off in enumerate(OFFS)
    ]
    for copy in code_copies:
        copy.wait_recv()
    lax.fori_loop(1, 8, lambda s, _: (build(s), 0)[1], 0)
    for copy in lx:
        copy.wait_recv()
    lsend[1] = lsend[0] + lrx[0] + lrx[1] + lrx[2]
    lc = start(remote(lsend.at[1], lrc, l_send.at[0, 3], l_recv.at[0, 3], {CORE: 1 - ci}))
    half = pl.ds(pl.multiple_of(ci * 16, 16), 16)

    quad = (lax.broadcasted_iota(jnp.int32, (256, 128), 1) // 32).astype(F32).astype(BF16)

    def group_sums(c, begin=0, end=8):
        if begin == 0:
            acc[...] = jnp.zeros_like(acc)

        def body(s, _):
            @pl.when(s > 0)
            def _():
                if c == 0:
                    for i in range(2):
                        part = recvb.at[0, s, pl.ds(i * 128, 128)]
                        remote(part, part, d_send.at[4 * i, s], d_recv.at[4 * i, s], y_peers[1]).wait_recv()
                else:
                    remote(recvb.at[c, s], recvb.at[c, s], d_send.at[c, s], d_recv.at[c, s], y_peers[1]).wait_recv()

            piece = recvb[c, s]
            x = piece.astype(F32)
            turned = [piece] + [pltpu.roll(x, 32 * d, 1).astype(BF16) for d in (1, 2, 3)]
            wide = []
            for k in range(4):
                spread = turned[(3 - k) % 4]
                for b in range(3):
                    spread = jnp.where(quad == b, turned[(b - k) % 4], spread)
                at_rows = pl.ds(k * 256, 256)
                wide.append(jnp.concatenate([spread * mask[s, at_rows, pl.ds(h * 128, 128)] for h in range(2)], axis=1))
            acc[...] += jnp.dot(onehot[s], jnp.concatenate(wide, axis=0), preferred_element_type=F32)
            return 0

        lax.fori_loop(begin, end, body, 0)

    near = (lax.broadcasted_iota(jnp.int32, (DONORS, 128), 1) & 16) == 0
    high_rows = [pl.ds(t * DONORS, DONORS) for t in range(3)]

    def send_sums(c):
        for t, at_rows in enumerate(high_rows):
            lower, upper = acc[at_rows, pl.ds(0, 128)], acc[at_rows, pl.ds(128, 128)]
            a = jnp.where(near, lower, pltpu.roll(upper, 16, 1))
            b = jnp.where(near, pltpu.roll(lower, 112, 1), upper)
            sums = (a, b) if c == 1 else (b, a)
            for d, off in enumerate((1, 3)):
                value = sums[d]
                if c == 2:
                    z_copies[0, d, t].wait_recv()
                    value = value + decoded(zrecv[0, d, at_rows, :])
                zsend[c, d, at_rows, :] = coded(value)
                z_copies[c, d, t] = start(
                    remote(
                        zsend.at[c, d, at_rows], zrecv.at[c, d, at_rows],
                        z_send.at[c, 3 * d + t], z_recv.at[c, 3 * d + t], {Z: moved(Z, off)},
                    )
                )

    def merged(a, b):
        return jnp.concatenate(
            [jnp.where(near, a, pltpu.roll(b, 16, 1)), jnp.where(near, pltpu.roll(a, 112, 1), b)], axis=1
        )

    z_copies = {}
    group_sums(0, 0, 4)
    lc.wait_recv()
    lsend[2] = lsend[1] + lrc[...]
    lz = [start(remote(lsend.at[2, half], lrz.at[k], l_send.at[1, k], l_recv.at[1, k], z_peers[k])) for k in range(1, 8)]
    group_sums(0, 4, 8)
    send_sums(0)
    for copy in g2:
        copy.wait_recv()
    g3 = [
        start(remote(gbuf.at[:, :, ci, quarter], gbuf.at[:, :, ci, quarter], g_send.at[2, o], g_recv.at[2, o], x_peers[o]))
        for o in range(3)
    ]

    group_sums(1)
    send_sums(1)
    for copy in lz:
        copy.wait_recv()
    half_lib[...] = lsend[2, half, :] + sum(lrz[k] for k in range(1, 8))
    ly = [
        start(remote(half_lib, lry.at[o], l_send.at[2, o], l_recv.at[2, o], {Y: moved(Y, off)}))
        for o, off in enumerate(OFFS)
    ]
    send_pieces(3)

    group_sums(2)
    send_sums(2)
    for copy in g3:
        copy.wait_recv()
    g4 = start(remote(gbuf.at[:, :, ci], gbuf.at[:, :, ci], g_send.at[3, 0], g_recv.at[3, 0], {CORE: 1 - ci}))

    for copy in ly:
        copy.wait_recv()
    library[half, :] = half_lib[...] + lry[0] + lry[1] + lry[2]
    ll = start(remote(library.at[half], library.at[half], l_send.at[2, 3], l_recv.at[2, 3], {CORE: 1 - ci}))

    group_sums(3, 0, 4)
    g4.wait_recv()
    geno_out = pltpu.make_async_copy(gbuf, geno_ref, out_sem.at[3])
    geno_out.start()
    ll.wait_recv()
    library_parts = three_parts(jnp.maximum(library[...], 1.0))
    type_row = lax.broadcasted_iota(jnp.int32, (32, 256), 0)
    tl = lax.broadcasted_iota(jnp.int32, (32, 256), 1) // 32
    for t, at_rows in enumerate(high_rows):
        expand = jnp.where(type_row == tl + 8 * t, 1.0, 0.0).astype(BF16)
        size = sum(lax.dot_general(part, expand, TN, preferred_element_type=F32) for part in library_parts)
        scale[at_rows, :] = 10000.0 / size
    for t, at_rows in enumerate(high_rows):
        for d in range(2):
            z_copies[1, d, t].wait_recv()
        acc[at_rows, :] += merged(decoded(zrecv[1, 0, at_rows, :]), decoded(zrecv[1, 1, at_rows, :]))
    group_sums(3, 4, 8)
    stores = [geno_out]
    for t in range(3):
        for d in range(2):
            z_copies[2, d, t].wait_recv()
    for t, at_rows in enumerate(high_rows):
        pseudo = acc[at_rows, :] + merged(decoded(zrecv[2, 1, at_rows, :]), decoded(zrecv[2, 0, at_rows, :]))
        logged = jnp.log1p(pseudo * scale[at_rows, :])
        spread = logged - jnp.mean(logged, axis=0, keepdims=True)
        standard = spread * lax.rsqrt(jnp.mean(spread * spread, axis=0, keepdims=True) + 1e-06)
        to_rows = pl.ds(t * 256, 256)
        std[to_rows, :] = jnp.transpose(standard).astype(BF16)
        stores.append(pltpu.make_async_copy(std.at[to_rows], std_ref.at[to_rows], out_sem.at[t]))
        stores[-1].start()
    for copy in stores:
        copy.wait()
    for copy in pending:
        copy.wait_send()


def scores_kernel(std_hbm, geno_hbm, out_ref, std_ref, geno_ref, buffer, in_sem, sem):
    loads = [pltpu.make_async_copy(std_hbm, std_ref, in_sem.at[len(BANDS)])]
    stores = []
    begin = 0
    for i, width in enumerate(BANDS):
        blocks = pl.ds(begin // 128, width // 128)
        loads.append(pltpu.make_async_copy(geno_hbm.at[blocks], geno_ref.at[blocks], in_sem.at[i]))
        columns = pl.ds(begin, width)
        stores.append(pltpu.make_async_copy(buffer.at[:, columns], out_ref.at[:, columns], sem.at[i]))
        begin += width
    for copy in loads:
        copy.start()
    loads[0].wait()
    begin = 0
    for i, width in enumerate(BANDS):
        loads[i + 1].wait()
        geno = jnp.concatenate([geno_ref[begin // 128 + j] for j in range(width // 128)], axis=1)
        product = jnp.dot(std_ref[...], geno, preferred_element_type=F32) * DONORS ** (-0.5)
        buffer[:, pl.ds(begin, width)] = product.astype(BF16)
        stores[i].start()
        begin += width
    for copy in stores:
        copy.wait()


def on_device(umi_counts, cell_donors, cell_types, live_cells, dosages):
    hbm = pl.BlockSpec(memory_space=pl.ANY)
    dma = pltpu.SemaphoreType.DMA
    standard, geno = pl.pallas_call(
        gather_kernel,
        name="gather",
        out_shape=(
            jax.ShapeDtypeStruct((768, 128), BF16),
            jax.ShapeDtypeStruct((4, 4, 2, 128, 128), BF16),
        ),
        in_specs=[pl.BlockSpec(memory_space=pltpu.SMEM)] + [hbm] * 4,
        out_specs=(hbm, hbm),
        scratch_shapes=[
            pltpu.VMEM((8, 128), jnp.int32),
            pltpu.VMEM((8, 128), jnp.int32),
            pltpu.VMEM((DONORS, 128), jnp.int32),
            pltpu.VMEM((768, 128), BF16),
            pltpu.VMEM((4, 1024, 256), jnp.int32),
            pltpu.VMEM((4, 8, 256, 128), BF16),
            pltpu.VMEM((4, 8, 256, 128), BF16),
            pltpu.VMEM((8, 8, 128), jnp.int32),
            pltpu.VMEM((8, 384, 1024), BF16),
            pltpu.VMEM((8, 1024, 256), BF16),
            pltpu.VMEM((384, 256), F32),
            pltpu.VMEM((3, 2, 384, 128), jnp.int16),
            pltpu.VMEM((3, 2, 384, 128), jnp.int16),
            pltpu.VMEM((256, 128), F32),
            pltpu.VMEM((128, 128), BF16),
            pltpu.VMEM((4, 4, 2, 128, 128), BF16),
            pltpu.VMEM((3, 32, 128), F32),
            pltpu.VMEM((3, 32, 128), F32),
            pltpu.VMEM((32, 128), F32),
            pltpu.VMEM((8, 16, 128), F32),
            pltpu.VMEM((3, 16, 128), F32),
            pltpu.VMEM((16, 128), F32),
            pltpu.VMEM((32, 128), F32),
            pltpu.VMEM((384, 256), F32),
            dma((11,)), dma((5, 8)), dma((5, 8)), dma((8,)), dma((8,)), dma((4, 3)), dma((4, 3)),
            dma((3, 8)), dma((3, 8)), dma((3, 6)), dma((3, 6)), dma((3,)), dma((4,)),
        ],
        compiler_params=pltpu.CompilerParams(
            collective_id=0, has_side_effects=True, vmem_limit_bytes=VMEM_LIMIT
        ),
    )(live_cells, umi_counts, cell_donors.reshape(8, 128), cell_types.reshape(8, 128), dosages)
    geno = geno.reshape(32, 128, 128)
    scores = pl.pallas_call(
        scores_kernel,
        name="scores",
        out_shape=jax.ShapeDtypeStruct((768, 4096), BF16),
        in_specs=[hbm, hbm],
        out_specs=hbm,
        scratch_shapes=[
            pltpu.VMEM((768, 128), BF16),
            pltpu.VMEM((32, 128, 128), BF16),
            pltpu.VMEM((768, 4096), BF16),
            dma((len(BANDS) + 1,)), dma((len(BANDS),)),
        ],
        compiler_params=pltpu.CompilerParams(vmem_limit_bytes=VMEM_LIMIT),
    )(standard, geno)
    return scores.reshape(TYPES, 32, 4096)


def solution(mesh):
    torus = Mesh(mesh.devices.reshape(*SIZES.values()), AXES)
    return jax.shard_map(
        on_device,
        mesh=torus,
        in_specs=(P(BATCH, GENE), P(BATCH), P(BATCH), P(BATCH), P(None, BATCH)),
        out_specs=P(None, GENE + BATCH, None),
        check_vma=False,
    )
```

```python
import jax
import jax.numpy as jnp
from jax import lax
from jax.experimental import pallas as pl
from jax.experimental.pallas import tpu as pltpu
from jax.sharding import Mesh
from jax.sharding import PartitionSpec as P

TYPES = 24
DONORS = 128
AXES = ("batch_0", "batch_1", "batch_2", "gene_0", "gene_1")
SIZES = {"batch_0": 4, "batch_1": 4, "batch_2": 2, "gene_0": 4, "gene_1": 2}
Z, Y, CORE, X, ZLO = AXES
BATCH = AXES[:3]
GENE = AXES[3:]
MESH = pl.DeviceIdType.MESH
F32 = jnp.float32
BF16 = jnp.bfloat16

BLOCKS = (2, 1, 3, 0)
CODE = 2112.0
LOG2 = 0.6931471805599453
SLOTS = tuple((dy, dc) for dy in (0, 2, 1, 3) for dc in (0, 1))
ZSLOTS = tuple((oz, ol) for oz in range(4) for ol in range(2))
OFFS = (1, 2, 3)
STRIP = 128
BANDS = (512, 512, 1024, 1024, 1024)
VMEM_LIMIT = 67043328
NT = (((1,), (1,)), ((), ()))
TN = (((0,), (0,)), ((), ()))


def three_parts(value):
    first = value.astype(BF16)
    rest = value - first.astype(F32)
    second = rest.astype(BF16)
    third = (rest - second.astype(F32)).astype(BF16)
    return first, second, third


def coded(sums):
    return ((jnp.log(1.0 + sums) * (CODE / LOG2) + 0.5).astype(jnp.int32) - 32768).astype(jnp.int16)


def decoded(codes):
    return jnp.exp((codes.astype(jnp.int32) + 32768).astype(F32) * (LOG2 / CODE)) - 1.0


def gather_kernel(
    live_ref, umi_ref, donors_hbm, types_hbm, dosages_hbm,
    std_ref, geno_ref,
    donors_ref, types_ref, dosages_ref, std,
    xin, sendb, recvb, codeb, onehot, mask, acc, zsend, zrecv, rows, gown, gbuf, lsend, lrx, lrc, lrz, lry, half_lib, library, scale,
    in_sem, d_send, d_recv, c_send, c_recv, g_send, g_recv, l_send, l_recv, z_send, z_recv, small_sem, out_sem,
):
    at = {axis: lax.axis_index(axis) for axis in AXES}
    zi, yi, ci, xi = at[Z], at[Y], at[CORE], at[X]

    def moved(axis, offset):
        return lax.rem(at[axis] + offset, SIZES[axis])

    def peer(**offsets):
        return {axis: moved(axis, offset) for axis, offset in offsets.items() if offset}

    def remote(src, dst, send, recv, device):
        return pltpu.make_async_remote_copy(
            src_ref=src, dst_ref=dst, send_sem=send, recv_sem=recv, device_id=device, device_id_type=MESH
        )

    y_peers = [peer(batch_1=dy, batch_2=dc) for dy, dc in SLOTS]
    z_peers = [peer(batch_0=oz, gene_1=ol) for oz, ol in ZSLOTS]
    x_peers = [peer(gene_0=o) for o in OFFS]

    def cells_of(block):
        return pl.ds(pl.multiple_of(block * 128, 128), 128)

    smalls = [
        pltpu.make_async_copy(src, dst, small_sem.at[i])
        for i, (src, dst) in enumerate(
            ((donors_hbm, donors_ref), (types_hbm, types_ref), (dosages_hbm, dosages_ref))
        )
    ]
    for copy in smalls:
        copy.start()
    loads = []
    col = pl.ds(pl.multiple_of(moved(Z, BLOCKS[0]) * 256, 256), 256)
    for i in range(2):
        for k in range(4):
            block = cells_of(2 * k + i)
            loads.append(pltpu.make_async_copy(umi_ref.at[block, col], xin.at[0, block], in_sem.at[4 * i + k]))
    for c in (1, 2, 3):
        col = pl.ds(pl.multiple_of(moved(Z, BLOCKS[c]) * 256, 256), 256)
        loads.append(pltpu.make_async_copy(umi_ref.at[:, col], xin.at[c], in_sem.at[7 + c]))
    for load in loads[:8]:
        load.start()

    barrier = pltpu.get_barrier_semaphore()
    for device in y_peers[1:] + z_peers[1:] + x_peers:
        pl.semaphore_signal(barrier, inc=1, device_id=device, device_id_type=MESH)

    rows[...] = jnp.zeros_like(rows)
    lane = lax.broadcasted_iota(jnp.int32, (STRIP, 128), 1)
    low = lane < 64
    even = (lane & 32) == 0
    first = (lane & 16) == 0

    def pack(c, begin=0, end=2):
        def body(i, _):
            r0 = pl.multiple_of(i * STRIP, STRIP)
            total = None
            for h in range(2):
                x = []
                for k in range(4):
                    cells = pl.ds(pl.multiple_of(k * 256 + r0, STRIP), STRIP)
                    value = xin[c, cells, pl.ds(h * 128, 128)]
                    if c in (1, 2):
                        value = jnp.where(first, value, xin[3 - c, cells, pl.ds(h * 128, 128)])
                    x.append(value.astype(F32))
                a = [None] * 4
                for k in range(2):
                    a[k] = jnp.where(low, x[k], pltpu.roll(x[k + 2], 64, 1))
                    a[k + 2] = jnp.where(low, pltpu.roll(x[k], 64, 1), x[k + 2])
                for k in (0, 2):
                    for q, piece in (
                        (k, jnp.where(even, a[k], pltpu.roll(a[k + 1], 32, 1))),
                        (k + 1, jnp.where(even, pltpu.roll(a[k], 96, 1), a[k + 1])),
                    ):
                        rounded = piece.astype(BF16)
                        sendb[c, h * 4 + q, pl.ds(r0, STRIP), :] = rounded
                        exact = rounded.astype(F32)
                        total = exact if total is None else total + exact
            rows[pl.ds(r0, STRIP), :] += total
            return 0

        lax.fori_loop(begin, end, body, 0)

    own = yi * 2 + ci
    pending = []

    def start(copy):
        copy.start()
        pending.append(copy)
        return copy

    def send_pieces(c):
        for k in (2, 3, 4, 5, 6, 7, 1):
            dy, dc = SLOTS[k]
            piece = moved(Y, dy) * 2 + moved(CORE, dc)
            start(remote(sendb.at[c, piece], recvb.at[c, k], d_send.at[c, k], d_recv.at[c, k], y_peers[k]))

    def send_half(i):
        at_rows = pl.ds(i * 128, 128)
        for k in (2, 3, 4, 5, 6, 7, 1):
            dy, dc = SLOTS[k]
            piece = moved(Y, dy) * 2 + moved(CORE, dc)
            start(
                remote(sendb.at[0, piece, at_rows], recvb.at[0, k, at_rows], d_send.at[4 * i, k], d_recv.at[4 * i, k], y_peers[k])
            )

    for load in loads[:4]:
        load.wait()
    for load in loads[8:]:
        load.start()
    pack(0, 0, 1)
    for copy in smalls:
        copy.wait()
    slot = lax.broadcasted_iota(jnp.int32, (8, 128), 0) * 128 + lax.broadcasted_iota(jnp.int32, (8, 128), 1)
    alive = slot < live_ref[0]
    types = types_ref[...]
    donors = donors_ref[...]
    codeb[0] = jnp.where(alive, ((types >> 3) * DONORS + donors) * 8 + (types & 7), -8)

    genotype = dosages_ref[...].astype(F32)
    centred = genotype - jnp.mean(genotype, axis=0, keepdims=True)
    gown[...] = (centred * lax.rsqrt(jnp.mean(centred * centred, axis=0, keepdims=True) + 1e-06)).astype(BF16)
    quarter = pl.ds(pl.multiple_of(xi * 32, 32), 32)
    gbuf[zi, yi, ci, quarter, :] = gown[quarter, :]
    pl.semaphore_wait(barrier, 7 + 7 + 3)
    code_copies = [
        start(remote(codeb.at[0], codeb.at[k], c_send.at[k], c_recv.at[k], y_peers[k])) for k in range(1, 8)
    ]
    g1 = [
        start(remote(gbuf.at[zi, yi, ci, quarter], gbuf.at[zi, yi, ci, quarter], g_send.at[0, o], g_recv.at[0, o], {Y: moved(Y, off)}))
        for o, off in enumerate(OFFS)
    ]
    send_half(0)
    for load in loads[4:8]:
        load.wait()
    pack(0, 1, 2)
    send_half(1)
    loads[8].wait()
    loads[9].wait()
    pack(1)
    send_pieces(1)
    pack(2)
    send_pieces(2)
    loads[10].wait()
    pack(3)
    for c in range(4):
        recvb[c, 0] = sendb[c, own]

    select = jnp.where(
        lax.broadcasted_iota(jnp.int32, (8, 128), 1) // 32 == lax.broadcasted_iota(jnp.int32, (8, 128), 0), 1.0, 0.0
    ).astype(BF16)
    sums = sum(lax.dot_general(select, part, NT, preferred_element_type=F32) for part in three_parts(rows[...]))
    part_library = None
    for k in range(4):
        type_row = jnp.concatenate([jnp.where(alive, types, -1)[2 * k + i : 2 * k + i + 1, :] for i in range(2)], axis=1)
        donor_row = jnp.concatenate([donors[2 * k + i : 2 * k + i + 1, :] for i in range(2)], axis=1)
        own_type = lax.broadcasted_iota(jnp.int32, (32, 256), 0) == type_row
        own_donor = jnp.where(lax.broadcasted_iota(jnp.int32, (DONORS, 256), 0) == donor_row, 1.0, 0.0).astype(BF16)
        for part in three_parts(sums[k : k + 1, :]):
            left = jnp.where(own_type, part.astype(F32), 0.0).astype(BF16)
            term = lax.dot_general(left, own_donor, NT, preferred_element_type=F32)
            part_library = term if part_library is None else part_library + term
    lsend[0] = part_library
    lx = [start(remote(lsend.at[0], lrx.at[o], l_send.at[0, o], l_recv.at[0, o], x_peers[o])) for o in range(3)]

    block = (lax.broadcasted_iota(jnp.int32, (128, 128), 1) // 32).astype(F32).astype(BF16)
    donor_at = lax.broadcasted_iota(jnp.int32, (128, 128), 0).astype(F32).astype(BF16)
    one, zero = jnp.ones((128, 128), BF16), jnp.zeros((128, 128), BF16)

    def down(row):
        return jnp.concatenate([jnp.broadcast_to(row, (16, 128)).astype(BF16)] * 8, axis=0)

    def build(s):
        code = codeb[s]
        columns = jnp.transpose((code & 7).astype(F32))
        donor = ((code >> 3) & 127).astype(F32)
        high = [jnp.where((code >> 10) == t, 1.0, 0.0) for t in range(3)]
        for g in range(8):
            cells = pl.ds(g * 128, 128)
            match = donor_at == down(donor[g : g + 1, :])
            for t in range(3):
                onehot[s, pl.ds(t * 128, 128), cells] = jnp.where(match, down(high[t][g : g + 1, :]), zero)
            column = jnp.broadcast_to(columns[:, g : g + 1], (128, 128)).astype(BF16)
            for h in range(2):
                mask[s, cells, pl.ds(h * 128, 128)] = jnp.where(column == block + 4 * h, one, zero)

    build(0)
    for copy in g1:
        copy.wait_recv()
    g2 = [
        start(remote(gbuf.at[zi, :, ci, quarter], gbuf.at[zi, :, ci, quarter], g_send.at[1, o], g_recv.at[1, o], {Z: moved(Z, off)}))
        for o, off in enumerate(OFFS)
    ]
    for copy in code_copies:
        copy.wait_recv()
    lax.fori_loop(1, 8, lambda s, _: (build(s), 0)[1], 0)
    for copy in lx:
        copy.wait_recv()
    lsend[1] = lsend[0] + lrx[0] + lrx[1] + lrx[2]
    lc = start(remote(lsend.at[1], lrc, l_send.at[0, 3], l_recv.at[0, 3], {CORE: 1 - ci}))
    half = pl.ds(pl.multiple_of(ci * 16, 16), 16)

    quad = (lax.broadcasted_iota(jnp.int32, (256, 128), 1) // 32).astype(F32).astype(BF16)

    wrapped = (3 - yi) // 3

    def group_sums(c, begin=0, end=8):
        if begin == 0:
            acc[...] = jnp.zeros_like(acc)

        def body(i, _):
            s = i + wrapped * (i // 4) * (2 - 4 * (i % 4 // 2))

            @pl.when(i > 0)
            def _():
                if c == 0:
                    for j in range(2):
                        part = recvb.at[0, s, pl.ds(j * 128, 128)]
                        remote(part, part, d_send.at[4 * j, s], d_recv.at[4 * j, s], y_peers[1]).wait_recv()
                else:
                    remote(recvb.at[c, s], recvb.at[c, s], d_send.at[c, s], d_recv.at[c, s], y_peers[1]).wait_recv()

            piece = recvb[c, s]
            x = piece.astype(F32)
            turned = [piece] + [pltpu.roll(x, 32 * d, 1).astype(BF16) for d in (1, 2, 3)]
            wide = []
            for k in range(4):
                spread = turned[(3 - k) % 4]
                for b in range(3):
                    spread = jnp.where(quad == b, turned[(b - k) % 4], spread)
                at_rows = pl.ds(k * 256, 256)
                wide.append(jnp.concatenate([spread * mask[s, at_rows, pl.ds(h * 128, 128)] for h in range(2)], axis=1))
            acc[...] += jnp.dot(onehot[s], jnp.concatenate(wide, axis=0), preferred_element_type=F32)
            return 0

        lax.fori_loop(begin, end, body, 0)

    near = (lax.broadcasted_iota(jnp.int32, (DONORS, 128), 1) & 16) == 0
    high_rows = [pl.ds(t * DONORS, DONORS) for t in range(3)]

    def send_sums(c):
        for t, at_rows in enumerate(high_rows):
            lower, upper = acc[at_rows, pl.ds(0, 128)], acc[at_rows, pl.ds(128, 128)]
            a = jnp.where(near, lower, pltpu.roll(upper, 16, 1))
            b = jnp.where(near, pltpu.roll(lower, 112, 1), upper)
            sums = (a, b) if c == 1 else (b, a)
            for d, off in enumerate((1, 3)):
                value = sums[d]
                if c == 2:
                    z_copies[0, d, t].wait_recv()
                    value = value + decoded(zrecv[0, d, at_rows, :])
                zsend[c, d, at_rows, :] = coded(value)
                z_copies[c, d, t] = start(
                    remote(
                        zsend.at[c, d, at_rows], zrecv.at[c, d, at_rows],
                        z_send.at[c, 3 * d + t], z_recv.at[c, 3 * d + t], {Z: moved(Z, off)},
                    )
                )

    def merged(a, b):
        return jnp.concatenate(
            [jnp.where(near, a, pltpu.roll(b, 16, 1)), jnp.where(near, pltpu.roll(a, 112, 1), b)], axis=1
        )

    z_copies = {}
    group_sums(0, 0, 4)
    lc.wait_recv()
    lsend[2] = lsend[1] + lrc[...]
    lz = [start(remote(lsend.at[2, half], lrz.at[k], l_send.at[1, k], l_recv.at[1, k], z_peers[k])) for k in range(1, 8)]
    group_sums(0, 4, 8)
    send_sums(0)
    for copy in g2:
        copy.wait_recv()
    g3 = [
        start(remote(gbuf.at[:, :, ci, quarter], gbuf.at[:, :, ci, quarter], g_send.at[2, o], g_recv.at[2, o], x_peers[o]))
        for o in range(3)
    ]

    group_sums(1)
    send_sums(1)
    for copy in lz:
        copy.wait_recv()
    half_lib[...] = lsend[2, half, :] + sum(lrz[k] for k in range(1, 8))
    ly = [
        start(remote(half_lib, lry.at[o], l_send.at[2, o], l_recv.at[2, o], {Y: moved(Y, off)}))
        for o, off in enumerate(OFFS)
    ]
    send_pieces(3)

    group_sums(2)
    send_sums(2)
    for copy in g3:
        copy.wait_recv()
    g4 = start(remote(gbuf.at[:, :, ci], gbuf.at[:, :, ci], g_send.at[3, 0], g_recv.at[3, 0], {CORE: 1 - ci}))

    for copy in ly:
        copy.wait_recv()
    library[half, :] = half_lib[...] + lry[0] + lry[1] + lry[2]
    ll = start(remote(library.at[half], library.at[half], l_send.at[2, 3], l_recv.at[2, 3], {CORE: 1 - ci}))

    group_sums(3, 0, 4)
    g4.wait_recv()
    geno_out = pltpu.make_async_copy(gbuf, geno_ref, out_sem.at[3])
    geno_out.start()
    ll.wait_recv()
    library_parts = three_parts(jnp.maximum(library[...], 1.0))
    type_row = lax.broadcasted_iota(jnp.int32, (32, 256), 0)
    tl = lax.broadcasted_iota(jnp.int32, (32, 256), 1) // 32
    for t, at_rows in enumerate(high_rows):
        expand = jnp.where(type_row == tl + 8 * t, 1.0, 0.0).astype(BF16)
        size = sum(lax.dot_general(part, expand, TN, preferred_element_type=F32) for part in library_parts)
        scale[at_rows, :] = 10000.0 / size
    for t, at_rows in enumerate(high_rows):
        for d in range(2):
            z_copies[1, d, t].wait_recv()
        acc[at_rows, :] += merged(decoded(zrecv[1, 0, at_rows, :]), decoded(zrecv[1, 1, at_rows, :]))
    group_sums(3, 4, 8)
    stores = [geno_out]
    for t in range(3):
        for d in range(2):
            z_copies[2, d, t].wait_recv()
    for t, at_rows in enumerate(high_rows):
        pseudo = acc[at_rows, :] + merged(decoded(zrecv[2, 1, at_rows, :]), decoded(zrecv[2, 0, at_rows, :]))
        logged = jnp.log1p(pseudo * scale[at_rows, :])
        spread = logged - jnp.mean(logged, axis=0, keepdims=True)
        standard = spread * lax.rsqrt(jnp.mean(spread * spread, axis=0, keepdims=True) + 1e-06)
        to_rows = pl.ds(t * 256, 256)
        std[to_rows, :] = jnp.transpose(standard).astype(BF16)
        stores.append(pltpu.make_async_copy(std.at[to_rows], std_ref.at[to_rows], out_sem.at[t]))
        stores[-1].start()
    for copy in stores:
        copy.wait()
    for copy in pending:
        copy.wait_send()


def scores_kernel(std_hbm, geno_hbm, out_ref, std_ref, geno_ref, buffer, in_sem, sem):
    loads = [pltpu.make_async_copy(std_hbm, std_ref, in_sem.at[len(BANDS)])]
    stores = []
    begin = 0
    for i, width in enumerate(BANDS):
        blocks = pl.ds(begin // 128, width // 128)
        loads.append(pltpu.make_async_copy(geno_hbm.at[blocks], geno_ref.at[blocks], in_sem.at[i]))
        columns = pl.ds(begin, width)
        stores.append(pltpu.make_async_copy(buffer.at[:, columns], out_ref.at[:, columns], sem.at[i]))
        begin += width
    for copy in loads:
        copy.start()
    loads[0].wait()
    begin = 0
    for i, width in enumerate(BANDS):
        loads[i + 1].wait()
        geno = jnp.concatenate([geno_ref[begin // 128 + j] for j in range(width // 128)], axis=1)
        product = jnp.dot(std_ref[...], geno, preferred_element_type=F32) * DONORS ** (-0.5)
        buffer[:, pl.ds(begin, width)] = product.astype(BF16)
        stores[i].start()
        begin += width
    for copy in stores:
        copy.wait()


def on_device(umi_counts, cell_donors, cell_types, live_cells, dosages):
    hbm = pl.BlockSpec(memory_space=pl.ANY)
    dma = pltpu.SemaphoreType.DMA
    standard, geno = pl.pallas_call(
        gather_kernel,
        name="gather",
        out_shape=(
            jax.ShapeDtypeStruct((768, 128), BF16),
            jax.ShapeDtypeStruct((4, 4, 2, 128, 128), BF16),
        ),
        in_specs=[pl.BlockSpec(memory_space=pltpu.SMEM)] + [hbm] * 4,
        out_specs=(hbm, hbm),
        scratch_shapes=[
            pltpu.VMEM((8, 128), jnp.int32),
            pltpu.VMEM((8, 128), jnp.int32),
            pltpu.VMEM((DONORS, 128), jnp.int32),
            pltpu.VMEM((768, 128), BF16),
            pltpu.VMEM((4, 1024, 256), jnp.int32),
            pltpu.VMEM((4, 8, 256, 128), BF16),
            pltpu.VMEM((4, 8, 256, 128), BF16),
            pltpu.VMEM((8, 8, 128), jnp.int32),
            pltpu.VMEM((8, 384, 1024), BF16),
            pltpu.VMEM((8, 1024, 256), BF16),
            pltpu.VMEM((384, 256), F32),
            pltpu.VMEM((3, 2, 384, 128), jnp.int16),
            pltpu.VMEM((3, 2, 384, 128), jnp.int16),
            pltpu.VMEM((256, 128), F32),
            pltpu.VMEM((128, 128), BF16),
            pltpu.VMEM((4, 4, 2, 128, 128), BF16),
            pltpu.VMEM((3, 32, 128), F32),
            pltpu.VMEM((3, 32, 128), F32),
            pltpu.VMEM((32, 128), F32),
            pltpu.VMEM((8, 16, 128), F32),
            pltpu.VMEM((3, 16, 128), F32),
            pltpu.VMEM((16, 128), F32),
            pltpu.VMEM((32, 128), F32),
            pltpu.VMEM((384, 256), F32),
            dma((11,)), dma((5, 8)), dma((5, 8)), dma((8,)), dma((8,)), dma((4, 3)), dma((4, 3)),
            dma((3, 8)), dma((3, 8)), dma((3, 6)), dma((3, 6)), dma((3,)), dma((4,)),
        ],
        compiler_params=pltpu.CompilerParams(
            collective_id=0, has_side_effects=True, vmem_limit_bytes=VMEM_LIMIT
        ),
    )(live_cells, umi_counts, cell_donors.reshape(8, 128), cell_types.reshape(8, 128), dosages)
    geno = geno.reshape(32, 128, 128)
    scores = pl.pallas_call(
        scores_kernel,
        name="scores",
        out_shape=jax.ShapeDtypeStruct((768, 4096), BF16),
        in_specs=[hbm, hbm],
        out_specs=hbm,
        scratch_shapes=[
            pltpu.VMEM((768, 128), BF16),
            pltpu.VMEM((32, 128, 128), BF16),
            pltpu.VMEM((768, 4096), BF16),
            dma((len(BANDS) + 1,)), dma((len(BANDS),)),
        ],
        compiler_params=pltpu.CompilerParams(vmem_limit_bytes=VMEM_LIMIT),
    )(standard, geno)
    return scores.reshape(TYPES, 32, 4096)


def solution(mesh):
    torus = Mesh(mesh.devices.reshape(*SIZES.values()), AXES)
    return jax.shard_map(
        on_device,
        mesh=torus,
        in_specs=(P(BATCH, GENE), P(BATCH), P(BATCH), P(BATCH), P(None, BATCH)),
        out_specs=P(None, GENE + BATCH, None),
        check_vma=False,
    )
```
